128 devices in a mesh: dp: 1, ep: 128 (over z, y, x, core).
Axes of the slice: x: 4, y: 4, z: 4, core: 2. Of those that a mesh axis runs over, the one named last changes fastest.
Arguments:
- hidden: bfloat16 [2048, 2048], P(('dp', 'ep'))
- k_cache: bfloat16 [2048, 32, 4, 128], P(('dp', 'ep'))
- v_cache: bfloat16 [2048, 32, 4, 128], P(('dp', 'ep'))
- seq_lens: int32 [2048], P(('dp', 'ep'))
- expert_ids: int32 [2048, 8], P(('dp', 'ep'))
- ln_attn: bfloat16 [2048], replicated
- w_q: bfloat16 [2048, 4096], replicated
- w_k: bfloat16 [2048, 512], replicated
- w_v: bfloat16 [2048, 512], replicated
- q_gain: bfloat16 [128], replicated
- k_gain: bfloat16 [128], replicated
- w_o: bfloat16 [4096, 2048], replicated
- ln_moe: bfloat16 [2048], replicated
- w_router: bfloat16 [2048, 128], replicated
- w_gate: bfloat16 [128, 2048, 768], P('ep')
- w_up: bfloat16 [128, 2048, 768], P('ep')
- w_down: bfloat16 [128, 768, 2048], P('ep')
Outputs:
- output 1: bfloat16 [2048, 2048], P(('dp', 'ep'))
- output 2: bfloat16 [2048, 32, 4, 128], P(('dp', 'ep'))
- output 3: bfloat16 [2048, 32, 4, 128], P(('dp', 'ep'))
All inputs are finite; a program needn't handle non-finite values.
Results may differ from the reference program's by a relative error of at most 0.00575958.
Values are sent between devices in bfloat16 or wider.
A program may use at most 1 GiB of HBM per device.

```python
import jax
import jax.numpy as jnp
import numpy as np
from jax import lax

D = 2048
HEADS = 32
KV_HEADS = 4
HEAD = 128
EXPERTS = 128
FF = 768
TOP = 8
ROPE_BASE = 1000000
TMAX = 32
SEQ_DEV = 16
GROUP = 128

BATCH = SEQ_DEV * GROUP
CAP = 2 * SEQ_DEV // (EXPERTS // TOP)
EPS = 1e-6


def draw_routing(route_key):
    group_width = EXPERTS // TOP
    pos_table = np.array([0 if tok_num < CAP else 1 + (tok_num - CAP) % (group_width - 1) for tok_num in range(SEQ_DEV)], dtype=np.int32)
    perm_key, tok_key = jax.random.split(route_key)
    expert_perm = jax.random.permutation(perm_key, EXPERTS).astype(jnp.int32)
    tok_keys = jax.random.split(tok_key, GROUP * TOP)
    tok_perms = jax.vmap(lambda one_key: jax.random.permutation(one_key, SEQ_DEV))(tok_keys)
    positions = jnp.asarray(pos_table)[tok_perms].reshape(GROUP, TOP, SEQ_DEV)
    offsets = (jnp.arange(TOP, dtype=jnp.int32) * group_width)[None, :, None]
    chosen_ids = expert_perm[offsets + positions]
    return jnp.transpose(chosen_ids, (0, 2, 1)).reshape(BATCH, TOP).astype(jnp.int32)


def draw_lens(len_key):
    spread_key, raw_key = jax.random.split(len_key)
    spread = jax.random.randint(spread_key, (GROUP, 1), 1, 5)
    raw_lens = jax.random.randint(raw_key, (GROUP, SEQ_DEV), 0, TMAX)
    seq_lens = (raw_lens * spread // 4).reshape(BATCH)
    return seq_lens.at[0].set(TMAX - 1).astype(jnp.int32)


def setup_inputs(seed: int = 0, part: int = 0) -> dict:
    base_key = jax.random.key(seed)
    shared_keys = jax.random.split(base_key, 12)
    part_keys = jax.random.split(jax.random.fold_in(base_key, part), 5)
    hidden = jax.random.normal(part_keys[0], (BATCH, D), jnp.float32).astype(jnp.bfloat16)
    k_cache = (1.5 * jax.random.normal(part_keys[1], (BATCH, TMAX, KV_HEADS, HEAD), jnp.float32)).astype(jnp.bfloat16)
    v_cache = jax.random.normal(part_keys[2], (BATCH, TMAX, KV_HEADS, HEAD), jnp.float32).astype(jnp.bfloat16)
    seq_lens = draw_lens(part_keys[3])
    expert_ids = draw_routing(part_keys[4])
    ln_attn = (1.0 + 0.2 * jax.random.normal(shared_keys[0], (D,), jnp.float32)).astype(jnp.bfloat16)
    w_q = (jax.random.normal(shared_keys[1], (D, HEADS * HEAD), jnp.float32) * D ** -0.5).astype(jnp.bfloat16)
    w_k = (jax.random.normal(shared_keys[2], (D, KV_HEADS * HEAD), jnp.float32) * D ** -0.5).astype(jnp.bfloat16)
    w_v = (jax.random.normal(shared_keys[3], (D, KV_HEADS * HEAD), jnp.float32) * D ** -0.5).astype(jnp.bfloat16)
    q_gain = (1.6 + 0.3 * jax.random.normal(shared_keys[4], (HEAD,), jnp.float32)).astype(jnp.bfloat16)
    k_gain = (1.6 + 0.3 * jax.random.normal(shared_keys[5], (HEAD,), jnp.float32)).astype(jnp.bfloat16)
    w_o = (jax.random.normal(shared_keys[6], (HEADS * HEAD, D), jnp.float32) * (HEADS * HEAD) ** -0.5).astype(jnp.bfloat16)
    ln_moe = (1.0 + 0.2 * jax.random.normal(shared_keys[7], (D,), jnp.float32)).astype(jnp.bfloat16)
    w_router = (2.0 * jax.random.normal(shared_keys[8], (D, EXPERTS), jnp.float32) * D ** -0.5).astype(jnp.bfloat16)
    w_gate = (jax.random.normal(shared_keys[9], (EXPERTS, D, FF), jnp.float32) * D ** -0.5).astype(jnp.bfloat16)
    w_up = (jax.random.normal(shared_keys[10], (EXPERTS, D, FF), jnp.float32) * D ** -0.5).astype(jnp.bfloat16)
    w_down = (2.0 * jax.random.normal(shared_keys[11], (EXPERTS, FF, D), jnp.float32) * FF ** -0.5).astype(jnp.bfloat16)
    return {'hidden': hidden, 'k_cache': k_cache, 'v_cache': v_cache, 'seq_lens': seq_lens, 'expert_ids': expert_ids, 'ln_attn': ln_attn, 'w_q': w_q, 'w_k': w_k, 'w_v': w_v, 'q_gain': q_gain, 'k_gain': k_gain, 'w_o': w_o, 'ln_moe': ln_moe, 'w_router': w_router, 'w_gate': w_gate, 'w_up': w_up, 'w_down': w_down}


def rms_scale(values, gain_vec):
    mean_sq = jnp.mean(values * values, axis=-1, keepdims=True)
    return values * lax.rsqrt(mean_sq + EPS) * gain_vec.astype(jnp.float32)


def rotate_half(values, angles):
    half_dim = values.shape[-1] // 2
    x_low = values[..., :half_dim]
    x_high = values[..., half_dim:]
    cos_val = jnp.cos(angles)
    sin_val = jnp.sin(angles)
    return jnp.concatenate([x_low * cos_val - x_high * sin_val, x_high * cos_val + x_low * sin_val], axis=-1)


def attend(hidden, k_cache, v_cache, seq_lens, ln_attn, w_q, w_k, w_v, q_gain, k_gain, w_o):
    n_seq = hidden.shape[0]
    h_f32 = hidden.astype(jnp.float32)
    x_norm = rms_scale(h_f32, ln_attn).astype(jnp.bfloat16)
    q_proj = jnp.dot(x_norm, w_q, preferred_element_type=jnp.float32).reshape(n_seq, HEADS, HEAD)
    k_proj = jnp.dot(x_norm, w_k, preferred_element_type=jnp.float32).reshape(n_seq, KV_HEADS, HEAD)
    v_new = jnp.dot(x_norm, w_v, preferred_element_type=jnp.float32).astype(jnp.bfloat16).reshape(n_seq, KV_HEADS, HEAD)
    inv_freq = jnp.power(float(ROPE_BASE), -jnp.arange(0, HEAD, 2).astype(jnp.float32) / HEAD)
    angles = seq_lens.astype(jnp.float32)[:, None, None] * inv_freq[None, None, :]
    q_rot = rotate_half(rms_scale(q_proj, q_gain), angles).astype(jnp.bfloat16)
    k_new = rotate_half(rms_scale(k_proj, k_gain), angles).astype(jnp.bfloat16)
    positions = jnp.arange(TMAX, dtype=jnp.int32)
    at_slot = (positions[None, :] == seq_lens[:, None])[:, :, None, None]
    k_all = jnp.where(at_slot, k_new[:, None], k_cache)
    v_all = jnp.where(at_slot, v_new[:, None], v_cache)
    q_grp = q_rot.reshape(n_seq, KV_HEADS, HEADS // KV_HEADS, HEAD)
    scores = jnp.einsum('skgd,stkd->skgt', q_grp.astype(jnp.float32), k_all.astype(jnp.float32)) * (HEAD ** -0.5)
    visible = (positions[None, :] <= seq_lens[:, None])[:, None, None, :]
    scores = jnp.where(visible, scores, -1e30)
    att_probs = jax.nn.softmax(scores, axis=-1).astype(jnp.bfloat16)
    attn_out = jnp.einsum('skgt,stkd->skgd', att_probs.astype(jnp.float32), v_all.astype(jnp.float32))
    attn_out = attn_out.astype(jnp.bfloat16).reshape(n_seq, HEADS * HEAD)
    y_res = h_f32 + jnp.dot(attn_out, w_o, preferred_element_type=jnp.float32)
    return y_res, k_all, v_all


def reference(hidden, k_cache, v_cache, seq_lens, expert_ids, ln_attn, w_q, w_k, w_v, q_gain, k_gain, w_o, ln_moe, w_router, w_gate, w_up, w_down):
    def block_attn(block_in):
        h_blk, kc_blk, vc_blk, len_blk = block_in
        return attend(h_blk, kc_blk, vc_blk, len_blk, ln_attn, w_q, w_k, w_v, q_gain, k_gain, w_o)

    y_blocks, k_blocks, v_blocks = lax.map(block_attn, (hidden.reshape(GROUP, SEQ_DEV, D), k_cache.reshape(GROUP, SEQ_DEV, TMAX, KV_HEADS, HEAD), v_cache.reshape(GROUP, SEQ_DEV, TMAX, KV_HEADS, HEAD), seq_lens.reshape(GROUP, SEQ_DEV)))
    y_res = y_blocks.reshape(BATCH, D)
    k_all = k_blocks.reshape(BATCH, TMAX, KV_HEADS, HEAD)
    v_all = v_blocks.reshape(BATCH, TMAX, KV_HEADS, HEAD)

    r_norm = rms_scale(y_res, ln_moe).astype(jnp.bfloat16)
    logits = jnp.dot(r_norm, w_router, preferred_element_type=jnp.float32)
    gate_vals = jax.nn.softmax(jnp.take_along_axis(logits, expert_ids, axis=1), axis=-1)

    n_pairs = BATCH * TOP
    per_expert = GROUP * CAP
    flat_ids = expert_ids.reshape(n_pairs)
    sort_order = jnp.argsort(flat_ids, stable=True)
    sorted_tok = (sort_order // TOP).astype(jnp.int32)
    counts = jnp.bincount(flat_ids, length=EXPERTS).astype(jnp.int32)
    starts = jnp.cumsum(counts) - counts
    tok_padded = jnp.concatenate([sorted_tok, jnp.zeros((per_expert,), jnp.int32)])

    def run_expert(expert_in):
        start_at, w_gate_e, w_up_e, w_down_e = expert_in
        tok_idx = lax.dynamic_slice(tok_padded, (start_at,), (per_expert,))
        tok_rows = jnp.take(r_norm, tok_idx, axis=0)
        gate_pre = jnp.dot(tok_rows, w_gate_e, preferred_element_type=jnp.float32)
        up_pre = jnp.dot(tok_rows, w_up_e, preferred_element_type=jnp.float32)
        hidden_act = (jax.nn.silu(gate_pre) * up_pre).astype(jnp.bfloat16)
        return jnp.dot(hidden_act, w_down_e, preferred_element_type=jnp.float32).astype(jnp.bfloat16)

    expert_out = lax.map(run_expert, (starts, w_gate, w_up, w_down))
    inverse = jnp.argsort(sort_order)
    pair_rank = inverse - starts[flat_ids]
    picked = expert_out[flat_ids, pair_rank].reshape(BATCH, TOP, D).astype(jnp.float32)
    moe_out = jnp.sum(gate_vals[:, :, None] * picked, axis=1)
    return (y_res + moe_out).astype(jnp.bfloat16), k_all, v_all
```

```python
import functools

import jax
import jax.numpy as jnp
import numpy as np
from jax import lax
from jax.experimental import pallas as pl
from jax.experimental.pallas import tpu as pltpu
from jax.sharding import PartitionSpec as P

MESH = pl.DeviceIdType.MESH
EPS = 1e-6
ROPE_BASE = 1000000.0
BF = jnp.bfloat16
F32 = jnp.float32
N = 128
S = 16
D = 2048
HD = 128
T = 32
NKV = 4
GQ = 8
FF = 768
CAP = 2
MIX = 37
GRP = 2


def offset_of(k):
    return (k * MIX) % N


def shift_dev(me, off, sign):
    c = (me % 2 + off) % 2
    x = (me // 2 % 4 + 4 + sign * (off // 2 % 4)) % 4
    y = (me // 8 % 4 + 4 + sign * (off // 8 % 4)) % 4
    z = (me // 32 + 4 + sign * (off // 32)) % 4
    return ((z * 4 + y) * 4 + x) * 2 + c


def rms_rope(v, gain, cos, sin):
    ms = jnp.mean(v * v, axis=-1, keepdims=True)
    v = v * lax.rsqrt(ms + EPS) * gain
    return v * cos + pltpu.roll(v, 64, axis=1) * sin


def kernel(h_hbm, kc_hbm, vc_hbm, sl_hbm, ids_hbm, lna_hbm, wq_hbm, wk_hbm, wv_hbm, qg_hbm, kg_hbm, wo_hbm,
           lnm_hbm, wr_hbm, wg_hbm, wu_hbm, wd_hbm, freq_hbm,
           out_ref, ko_hbm, vo_hbm,
           h_v, sl_s, ids_v, lna_v, lnm_v, qg_v, kg_v, freq_v,
           wk_v, wv_v, wq_v, wo_v, wr_v, wg_v, wu_v, wd_v,
           kc_v, vc_v, kp_v, vp_v, x_v, kn_v, mask_v, trig_v, at_v, y_v, r_v, p_v, snd_v, g_v, hid_v,
           sbuf, rbuf, obuf, bbuf,
           sm_small, sm_kv, sm_cache, sm_wq, sm_wo, sm_wr, sm_we, sm_out,
           ssem, osem, rsem, bsem):
    me = lax.axis_index("ep")
    cp = pltpu.make_async_copy

    small = [cp(a, b, sm_small.at[i]) for i, (a, b) in enumerate([
        (h_hbm, h_v), (lna_hbm, lna_v), (sl_hbm, sl_s), (freq_hbm, freq_v), (kg_hbm, kg_v), (qg_hbm, qg_v),
        (ids_hbm, ids_v), (lnm_hbm, lnm_v)])]
    for c in small:
        c.start()
    kvw = [cp(wk_hbm, wk_v, sm_kv.at[0]), cp(wv_hbm, wv_v, sm_kv.at[1])]
    caches = [cp(kc_hbm, kc_v, sm_cache.at[0]), cp(vc_hbm, vc_v, sm_cache.at[1])]

    def wq_copy(g):
        return cp(wq_hbm.at[:, pl.ds(pl.multiple_of(g * 1024, 1024), 1024)], wq_v.at[g], sm_wq.at[g])

    def wo_copy(n):
        return cp(wo_hbm.at[:, pl.ds(pl.multiple_of(n * 512, 512), 512)], wo_v.at[n], sm_wo.at[n])

    for c in kvw + caches:
        c.start()
    wq_copy(0).start()
    wq_copy(1).start()

    bar = pltpu.get_barrier_semaphore()

    @pl.loop(1, N)
    def _(k):
        pl.semaphore_signal(bar, inc=1, device_id={"ep": (me + k) % N}, device_id_type=MESH)

    for c in small:
        c.wait()

    lane = lax.broadcasted_iota(jnp.int32, (S, CAP * N), 1)
    off = ((lane >> 1) * MIX) & (N - 1)
    mc, mx, my, mz = me % 2, me // 2 % 4, me // 8 % 4, me // 32
    e_row = (((((mz + (off >> 5)) & 3) * 4 + ((my + ((off >> 3) & 3)) & 3)) * 4 + ((mx + ((off >> 1) & 3)) & 3)) * 2
             + ((mc + (off & 1)) & 1))
    ids = ids_v[...]
    chosen = jnp.zeros((S, CAP * N), F32)
    for k in range(8):
        chosen = chosen + jnp.where(ids[:, k:k + 1] == e_row, 1.0, 0.0)
    tri = jnp.where(lax.broadcasted_iota(jnp.int32, (S, S), 0) > lax.broadcasted_iota(jnp.int32, (S, S), 1), 1.0, 0.0)
    rank = jnp.dot(tri.astype(BF), chosen.astype(BF), preferred_element_type=F32)
    send = chosen * jnp.where(rank == (lane & 1).astype(F32), 1.0, 0.0)
    snd_v[...] = send
    p_v[...] = jnp.transpose(send).astype(BF)

    hf = h_v[...].astype(F32)
    rs = lax.rsqrt(jnp.mean(hf * hf, axis=-1, keepdims=True) + EPS)
    lna = lna_v[...].astype(F32)
    for j in range(16):
        sl = slice(j * 128, (j + 1) * 128)
        x_v[:, sl] = (hf[:, sl] * rs * lna[j:j + 1, :]).astype(BF)

    srow = lax.broadcasted_iota(jnp.int32, (S, 128), 0)
    lens = jnp.zeros((S, 128), jnp.int32)
    for s in range(S):
        lens = jnp.where(srow == s, sl_s[s], lens)
    ang = lens.astype(F32) * freq_v[...]
    sgn = jnp.where(lax.broadcasted_iota(jnp.int32, (S, 128), 1) < 64, -1.0, 1.0)
    cos = jnp.cos(ang)
    sin = jnp.sin(ang) * sgn
    trig_v[0] = cos
    trig_v[1] = sin
    for b in range(4):
        col = lax.broadcasted_iota(jnp.int32, (S, 128), 1) + b * 128
        ok = ((col >> 5) == srow) & ((col & 31) <= lens)
        mask_v[:, b * 128:(b + 1) * 128] = jnp.where(ok, 0.0, -1e30)

    x = x_v[...]
    kg = kg_v[...].astype(F32)
    kvw[0].wait()
    kp = jnp.dot(x, wk_v[...], preferred_element_type=F32)
    for g in range(NKV):
        kn_v[0, g] = rms_rope(kp[:, g * 128:(g + 1) * 128], kg, cos, sin)
    kvw[1].wait()
    vp = jnp.dot(x, wv_v[...], preferred_element_type=F32)
    for g in range(NKV):
        kn_v[1, g] = vp[:, g * 128:(g + 1) * 128]

    ri = lax.broadcasted_iota(jnp.int32, (256, 64), 0)
    ci = lax.broadcasted_iota(jnp.int32, (256, 64), 1)
    rep1 = jnp.where(((ri >> 4) == (ci & 15)) & ((ri & 3) == (ci >> 4)), 1.0, 0.0).astype(BF)
    pr = lax.broadcasted_iota(jnp.int32, (128, 128), 0)
    pc = lax.broadcasted_iota(jnp.int32, (128, 128), 1)
    perm = jnp.where(((pr & 31) == (pc >> 2)) & ((pr >> 5) == (pc & 3)), 1.0, 0.0).astype(BF)
    trow = pr >> 2
    for i, (buf, dst) in enumerate(((kc_v, kp_v), (vc_v, vp_v))):
        caches[i].wait()
        rows = buf.reshape(S * T * NKV, HD)
        new = jnp.concatenate([kn_v[i, g].astype(BF) for g in range(NKV)], axis=0)
        rep = jnp.dot(rep1, new, preferred_element_type=F32)
        for s in range(S):
            old = rows[s * 128:(s + 1) * 128, :].astype(F32)
            rep_s = jnp.concatenate([rep[s * 16:(s + 1) * 16, :]] * 8, axis=0)
            upd = jnp.where(trow == sl_s[s], rep_s, old).astype(BF)
            rows[s * 128:(s + 1) * 128, :] = upd
            grp = jnp.dot(perm, upd, preferred_element_type=F32).astype(BF)
            for g in range(NKV):
                dst[g, s * 32:(s + 1) * 32, :] = grp[g * 32:(g + 1) * 32, :]
    couts = [cp(kc_v, ko_hbm, sm_out.at[0]), cp(vc_v, vo_hbm, sm_out.at[1])]

    qg = qg_v[...].astype(F32)

    @pl.loop(0, NKV)
    def _(g):
        wq_copy(g).wait()

        @pl.when(g < 2)
        def _():
            wq_copy(g + 2).start()

        @pl.when(g >= 2)
        def _():
            wo_copy(g - 2).start()
        q = jnp.dot(x_v[...], wq_v[g], preferred_element_type=F32)
        q = jnp.concatenate([q[:, j * 128:(j + 1) * 128] for j in range(GQ)], axis=0)
        cs = jnp.concatenate([trig_v[0]] * GQ, axis=0)
        sn = jnp.concatenate([trig_v[1]] * GQ, axis=0)
        q = rms_rope(q, qg, cs, sn).astype(BF)
        sc = lax.dot_general(q, kp_v[g], (((1,), (1,)), ((), ())), preferred_element_type=F32)
        mk = mask_v[...]
        sc = jnp.where(jnp.concatenate([mk] * GQ, axis=0) == 0.0, sc * (HD ** -0.5), -1e30)
        ex = jnp.exp(sc - jnp.max(sc, axis=-1, keepdims=True))
        pb = (ex / jnp.sum(ex, axis=-1, keepdims=True)).astype(BF)
        o = jnp.dot(pb, vp_v[g], preferred_element_type=F32).astype(BF)
        for j in range(GQ):
            at_v[:, pl.ds(pl.multiple_of((g * GQ + j) * 128, 128), 128)] = o[j * S:(j + 1) * S, :]

    for c in couts:
        c.start()
    wr_c = cp(wr_hbm, wr_v, sm_wr)
    we_c = [cp(wg_hbm.at[0], wg_v, sm_we.at[0]), cp(wu_hbm.at[0], wu_v, sm_we.at[1]), cp(wd_hbm.at[0], wd_v, sm_we.at[2])]

    @pl.loop(0, 4)
    def _(n):
        wo_copy(n).wait()

        @pl.when(n < 2)
        def _():
            wo_copy(n + 2).start()

        @pl.when(n == 2)
        def _():
            wr_c.start()
            we_c[0].start()

        @pl.when(n == 3)
        def _():
            we_c[1].start()
            we_c[2].start()
        cols = pl.ds(pl.multiple_of(n * 512, 512), 512)
        y_v[:, cols] = h_v[:, cols].astype(F32) + jnp.dot(at_v[...], wo_v[n], preferred_element_type=F32)

    y = y_v[...]
    rs = lax.rsqrt(jnp.mean(y * y, axis=-1, keepdims=True) + EPS)
    lnm = lnm_v[...].astype(F32)
    for j in range(16):
        sl = slice(j * 128, (j + 1) * 128)
        r_v[:, sl] = (y[:, sl] * rs * lnm[j:j + 1, :]).astype(BF)

    sview, rview = sbuf.reshape(16, CAP * N, HD), rbuf.reshape(16, CAP * N, HD)
    oview, bview = obuf.reshape(16, CAP * N, HD), bbuf.reshape(16, CAP * N, HD)
    for n in range(4):
        rows = jnp.dot(p_v[...], r_v[:, n * 512:(n + 1) * 512], preferred_element_type=F32).astype(BF)
        for j in range(4):
            sview[n * 4 + j] = rows[:, j * 128:(j + 1) * 128]
    pl.semaphore_wait(bar, N - 1)
    gsz = N // GRP
    for q in range(GRP):
        @pl.loop(1 if q == 0 else q * gsz, (q + 1) * gsz)
        def _(k):
            pltpu.make_async_remote_copy(sbuf.at[:, k], rbuf.at[:, k], ssem, rsem.at[q],
                                         device_id={"ep": shift_dev(me, offset_of(k), 1)}, device_id_type=MESH).start()
    rbuf[:, 0] = sbuf[:, 0]

    wr_c.wait()
    logits = jnp.dot(r_v[...], wr_v[...], preferred_element_type=F32)
    lane2 = lax.broadcasted_iota(jnp.int32, (N, CAP * N), 1)
    off2 = ((lane2 >> 1) * MIX) & (N - 1)
    e2 = (((((mz + (off2 >> 5)) & 3) * 4 + ((my + ((off2 >> 3) & 3)) & 3)) * 4 + ((mx + ((off2 >> 1) & 3)) & 3)) * 2
          + ((mc + (off2 & 1)) & 1))
    expand = jnp.where(lax.broadcasted_iota(jnp.int32, (N, CAP * N), 0) == e2, 1.0, 0.0)
    lg = jnp.dot(logits, expand, precision=lax.Precision.HIGHEST, preferred_element_type=F32)
    on = snd_v[...] > 0.5
    top = jnp.max(jnp.where(on, lg, -jnp.inf), axis=-1, keepdims=True)
    ex = jnp.where(on, jnp.exp(jnp.where(on, lg - top, 0.0)), 0.0)
    gates = ex / jnp.sum(ex, axis=-1, keepdims=True)
    g1 = gates.astype(BF)
    d1 = gates - g1.astype(F32)
    g2 = d1.astype(BF)
    g3 = (d1 - g2.astype(F32)).astype(BF)
    g_v[...] = jnp.concatenate([g1, g2, g3], axis=0)
    for c in we_c:
        c.wait()

    rr = CAP * gsz
    for q in range(GRP):
        lo = 1 if q == 0 else q * gsz
        got = rbuf.at[:, pl.ds(lo, (q + 1) * gsz - lo)]
        cp(got, got, rsem.at[q]).wait()

        @pl.loop(0, FF // 256)
        def _(n):
            cols = pl.ds(pl.multiple_of(n * 256, 256), 256)
            ga = jnp.zeros((rr, 256), F32)
            ua = jnp.zeros((rr, 256), F32)
            for kk in range(8):
                xk = jnp.concatenate([rview[2 * kk, q * rr:(q + 1) * rr, :], rview[2 * kk + 1, q * rr:(q + 1) * rr, :]], axis=1)
                ga = ga + jnp.dot(xk, wg_v[kk * 256:(kk + 1) * 256, cols], preferred_element_type=F32)
                ua = ua + jnp.dot(xk, wu_v[kk * 256:(kk + 1) * 256, cols], preferred_element_type=F32)
            hid_v[q * rr:(q + 1) * rr, cols] = (jax.nn.silu(ga) * ua).astype(BF)

        @pl.loop(0, 4)
        def _(n):
            cols = pl.ds(pl.multiple_of(n * 512, 512), 512)
            o = jnp.dot(hid_v[q * rr:(q + 1) * rr, :], wd_v[:, cols], preferred_element_type=F32).astype(BF)
            for j in range(4):
                oview[n * 4 + j, q * rr:(q + 1) * rr, :] = o[:, j * 128:(j + 1) * 128]

        @pl.loop(lo, (q + 1) * gsz)
        def _(k):
            pltpu.make_async_remote_copy(obuf.at[:, k], bbuf.at[:, k], osem, bsem,
                                         device_id={"ep": shift_dev(me, offset_of(k), -1)}, device_id_type=MESH).start()
    bbuf[:, 0] = obuf[:, 0]

    got = bbuf.at[:, pl.ds(1, N - 1)]
    cp(got, got, bsem).wait()
    for n in range(4):
        back = jnp.concatenate([bview[n * 4 + j] for j in range(4)], axis=1)
        m = jnp.dot(g_v[...], back, preferred_element_type=F32)
        cols = slice(n * 512, (n + 1) * 512)
        out_ref[:, cols] = (y_v[:, cols] + (m[0:S] + m[S:2 * S] + m[2 * S:3 * S])).astype(BF)
    sent = sbuf.at[:, pl.ds(1, N - 1)]
    cp(sent, sent, ssem).wait()
    cp(sent, sent, osem).wait()
    for c in couts:
        c.wait()


def solution(mesh):
    row_spec = P(('dp', 'ep'), None)
    cache_spec = P(('dp', 'ep'), None, None, None)
    len_spec = P(('dp', 'ep'))
    rep_vec = P(None)
    rep_mat = P(None, None)
    exp_spec = P('ep', None, None)
    inv = np.power(ROPE_BASE, -np.arange(0, HD, 2).astype(np.float32) / HD).astype(np.float32)
    freq_np = np.concatenate([inv, inv])[None, :]
    dma = pltpu.SemaphoreType.DMA

    def local_step(hidden, k_cache, v_cache, seq_lens, expert_ids, ln_attn, w_q, w_k, w_v, q_gain, k_gain, w_o, ln_moe, w_router, w_gate, w_up, w_down):
        anyspec = pl.BlockSpec(memory_space=pl.ANY)
        V = pltpu.VMEM
        return pl.pallas_call(
            kernel,
            out_shape=(jax.ShapeDtypeStruct((S, D), BF),
                       jax.ShapeDtypeStruct((S, T, NKV, HD), BF), jax.ShapeDtypeStruct((S, T, NKV, HD), BF)),
            in_specs=[anyspec] * 18,
            out_specs=(pl.BlockSpec(memory_space=pltpu.VMEM), anyspec, anyspec),
            scratch_shapes=[
                V((S, D), BF), pltpu.SMEM((S,), jnp.int32), V((S, 8), jnp.int32), V((16, 128), BF), V((16, 128), BF),
                V((1, HD), BF), V((1, HD), BF), V((1, HD), F32),
                V((D, 512), BF), V((D, 512), BF), V((4, D, 1024), BF), V((4, 4096, 512), BF), V((D, N), BF),
                V((D, FF), BF), V((D, FF), BF), V((FF, D), BF),
                V((S, T, NKV, HD), BF), V((S, T, NKV, HD), BF), V((NKV, S * T, HD), BF), V((NKV, S * T, HD), BF),
                V((S, D), BF), V((2, NKV, S, HD), F32), V((S, S * T), F32), V((2, S, HD), F32), V((S, 4096), BF),
                V((S, D), F32), V((S, D), BF), V((CAP * N, S), BF), V((S, CAP * N), F32), V((3 * S, CAP * N), BF),
                V((CAP * N, FF), BF),
                V((16, N, CAP, HD), BF), V((16, N, CAP, HD), BF), V((16, N, CAP, HD), BF), V((16, N, CAP, HD), BF),
                dma((8,)), dma((2,)), dma((2,)), dma((4,)), dma((4,)), dma, dma((3,)), dma((2,)),
                dma, dma, dma((GRP,)), dma,
            ],
            compiler_params=pltpu.CompilerParams(collective_id=0, has_side_effects=True, vmem_limit_bytes=67043328),
        )(hidden, k_cache, v_cache, seq_lens, expert_ids, ln_attn.reshape(16, 128), w_q, w_k, w_v,
          q_gain.reshape(1, HD), k_gain.reshape(1, HD), w_o, ln_moe.reshape(16, 128), w_router, w_gate, w_up, w_down,
          jnp.asarray(freq_np))

    return jax.shard_map(local_step, mesh=mesh, in_specs=(row_spec, cache_spec, cache_spec, len_spec, row_spec, rep_vec, rep_mat, rep_mat, rep_mat, rep_vec, rep_vec, rep_mat, rep_vec, rep_mat, exp_spec, exp_spec, exp_spec), out_specs=(row_spec, cache_spec, cache_spec), check_vma=False)
```

```python
import functools

import jax
import jax.numpy as jnp
import numpy as np
from jax import lax
from jax.experimental import pallas as pl
from jax.experimental.pallas import tpu as pltpu
from jax.sharding import PartitionSpec as P

MESH = pl.DeviceIdType.MESH
EPS = 1e-6
ROPE_BASE = 1000000.0
BF = jnp.bfloat16
F32 = jnp.float32
N = 128
S = 16
D = 2048
HD = 128
T = 32
NKV = 4
GQ = 8
FF = 768
CAP = 2
GRP = 2
FIN = 2


def peers(me, t, sign):
    a, b = lax.div(t, 4), lax.rem(t, 4)
    c, x, y, z = lax.rem(me, 2), lax.rem(lax.div(me, 2), 4), lax.rem(lax.div(me, 8), 4), lax.div(me, 32)
    zs = [lax.rem(z + 8 + sign * (a + f), 4) * 32 for f in range(4)]
    ys = [lax.rem(y + 8 + sign * (b + g), 4) * 8 for g in range(4)]
    xs = [lax.rem(x + 4 + sign * d, 4) * 2 for d in range(4)]
    cs = [c, 1 - c]
    return [zs[i % 4] + ys[i // 2] + (xs[i // 2] + cs[i % 2]) for i in range(8)]


def rms_rope(v, gain, cos, sin):
    ms = jnp.mean(v * v, axis=-1, keepdims=True)
    v = v * lax.rsqrt(ms + EPS) * gain
    return v * cos + pltpu.roll(v, 64, axis=1) * sin


def kernel(h_hbm, kc_hbm, vc_hbm, sl_hbm, ids_hbm, lna_hbm, wq_hbm, wk_hbm, wv_hbm, qg_hbm, kg_hbm, wo_hbm,
           lnm_hbm, wr_hbm, wg_hbm, wu_hbm, wd_hbm, freq_hbm,
           out_ref, rep_ref,
           h_v, sl_s, ids_v, lna_v, lnm_v, qg_v, kg_v, freq_v,
           wk_v, wv_v, wq_v, wo_v, wr_v, wg_v, wu_v, wd_v,
           kc_v, vc_v, kp_v, vp_v, x_v, kn_v, mask_v, trig_v, at_v, yh_v, yp_v, y_v, r_v, p_v, snd_v, g_v, hid_v,
           sbuf, rbuf, obuf, bbuf,
           sm_small, sm_kv, sm_cache, sm_wq, sm_wo, sm_wr, sm_we, as_sem, ar_sem, ys_sem, yr_sem,
           ssem, osem, rsem, bsem):
    me = lax.axis_index("ep")
    cp = pltpu.make_async_copy
    half = me % 2
    mate = me + 1 - 2 * half

    small = [cp(a, b, sm_small.at[i]) for i, (a, b) in enumerate([
        (h_hbm, h_v), (lna_hbm, lna_v), (sl_hbm, sl_s), (freq_hbm, freq_v), (kg_hbm, kg_v), (qg_hbm, qg_v),
        (ids_hbm, ids_v), (lnm_hbm, lnm_v)])]
    for c in small:
        c.start()
    kvw = [cp(wk_hbm, wk_v, sm_kv.at[0]), cp(wv_hbm, wv_v, sm_kv.at[1])]
    caches = [cp(kc_hbm, kc_v, sm_cache.at[0]), cp(vc_hbm, vc_v, sm_cache.at[1])]

    def wq_copy(g):
        return cp(wq_hbm.at[:, pl.ds(pl.multiple_of(g * 1024, 1024), 1024)], wq_v.at[g], sm_wq.at[g])

    def wo_copy(n):
        return cp(wo_hbm.at[pl.ds(n * 1024, 1024), pl.ds(pl.multiple_of(half * 1024, 1024), 1024)], wo_v.at[n], sm_wo.at[n])

    wr_c = cp(wr_hbm, wr_v, sm_wr)
    we_c = [cp(wg_hbm.at[0], wg_v, sm_we.at[0]), cp(wu_hbm.at[0], wu_v, sm_we.at[1]), cp(wd_hbm.at[0], wd_v, sm_we.at[2])]
    for c in kvw + caches:
        c.start()
    wq_copy(0).start()

    bar = pltpu.get_barrier_semaphore()

    for i in range(8):
        pl.semaphore_signal(bar, inc=1, device_id={"ep": lax.rem(me + (i + 1), N)}, device_id_type=MESH)

    @pl.loop(0, 7)
    def _(b):
        base = me + b * 17
        for i in range(17):
            pl.semaphore_signal(bar, inc=1, device_id={"ep": lax.rem(base + (i + 9), N)}, device_id_type=MESH)

    for c in small:
        c.wait()

    wq_copy(1).start()
    wq_copy(2).start()

    hf = h_v[...].astype(F32)
    rs = lax.rsqrt(jnp.mean(hf * hf, axis=-1, keepdims=True) + EPS)
    lna = lna_v[...].astype(F32)
    for j in range(16):
        sl = slice(j * 128, (j + 1) * 128)
        x_v[:, sl] = (hf[:, sl] * rs * lna[j:j + 1, :]).astype(BF)

    srow = lax.broadcasted_iota(jnp.int32, (S, 128), 0)
    lens = jnp.zeros((S, 128), jnp.int32)
    for s in range(S):
        lens = jnp.where(srow == s, sl_s[s], lens)
    ang = lens.astype(F32) * freq_v[...]
    sgn = jnp.where(lax.broadcasted_iota(jnp.int32, (S, 128), 1) < 64, -1.0, 1.0)
    cos = jnp.cos(ang)
    sin = jnp.sin(ang) * sgn
    trig_v[0] = cos
    trig_v[1] = sin
    for b in range(4):
        col = lax.broadcasted_iota(jnp.int32, (S, 128), 1) + b * 128
        ok = ((col >> 5) == srow) & ((col & 31) <= lens)
        mask_v[:, b * 128:(b + 1) * 128] = jnp.where(ok, 0.0, -1e30)

    x = x_v[...]
    kg = kg_v[...].astype(F32)
    kvw[0].wait()
    kp = jnp.dot(x, wk_v[...], preferred_element_type=F32)
    for g in range(NKV):
        kn_v[0, g] = rms_rope(kp[:, g * 128:(g + 1) * 128], kg, cos, sin)
    kvw[1].wait()
    vp = jnp.dot(x, wv_v[...], preferred_element_type=F32)
    for g in range(NKV):
        kn_v[1, g] = vp[:, g * 128:(g + 1) * 128]

    wq_copy(3).start()

    ri = lax.broadcasted_iota(jnp.int32, (256, 64), 0)
    ci = lax.broadcasted_iota(jnp.int32, (256, 64), 1)
    rep1 = jnp.where(((ri >> 4) == (ci & 15)) & ((ri & 3) == (ci >> 4)), 1.0, 0.0).astype(BF)
    pr = lax.broadcasted_iota(jnp.int32, (128, 128), 0)
    pc = lax.broadcasted_iota(jnp.int32, (128, 128), 1)
    perm = jnp.where(((pr & 31) == (pc >> 2)) & ((pr >> 5) == (pc & 3)), 1.0, 0.0).astype(BF)
    trow = pr >> 2
    for i, (buf, dst) in enumerate(((kc_v, kp_v), (vc_v, vp_v))):
        caches[i].wait()
        rows = buf.reshape(S * T * NKV, HD)
        new = jnp.concatenate([kn_v[i, g].astype(BF) for g in range(NKV)], axis=0)
        rep = jnp.dot(rep1, new, preferred_element_type=F32)
        rep_ref[i] = rep.astype(BF)
        for s in range(S):
            old = rows[s * 128:(s + 1) * 128, :].astype(F32)
            rep_s = jnp.concatenate([rep[s * 16:(s + 1) * 16, :]] * 8, axis=0)
            upd = jnp.where(trow == sl_s[s], rep_s, old).astype(BF)
            grp = jnp.dot(perm, upd, preferred_element_type=F32).astype(BF)
            for g in range(NKV):
                dst[g, s * 32:(s + 1) * 32, :] = grp[g * 32:(g + 1) * 32, :]

    def at_copy(g):
        return pltpu.make_async_remote_copy(at_v.at[g, pl.ds(0, S)], at_v.at[g, pl.ds(S, S)], as_sem.at[g], ar_sem.at[g],
                                            device_id={"ep": mate}, device_id_type=MESH)
    pl.semaphore_wait(bar, N - 1)

    qg = qg_v[...].astype(F32)

    def attend(g, q):
        sc = lax.dot_general(q, kp_v[g], (((1,), (1,)), ((), ())), preferred_element_type=F32)
        mk = mask_v[...]
        sc = jnp.where(jnp.concatenate([mk] * GQ, axis=0) == 0.0, sc * (HD ** -0.5), -1e30)
        ex = jnp.exp(sc - jnp.max(sc, axis=-1, keepdims=True))
        pb = (ex / jnp.sum(ex, axis=-1, keepdims=True)).astype(BF)
        o = jnp.dot(pb, vp_v[g], preferred_element_type=F32).astype(BF)
        for j in range(GQ):
            at_v[g, 0:S, j * 128:(j + 1) * 128] = o[j * S:(j + 1) * S, :]

    prev = None
    for g in range(NKV):
        wq_copy(g).wait()
        if g == 0:
            wo_copy(0).start()
            wo_copy(1).start()
        elif g < 3:
            wo_copy(g + 1).start()
        else:
            wr_c.start()
            we_c[0].start()
        q = jnp.dot(x_v[...], wq_v[g], preferred_element_type=F32)
        if g:
            attend(g - 1, prev)
        q = jnp.concatenate([q[:, j * 128:(j + 1) * 128] for j in range(GQ)], axis=0)
        cs = jnp.concatenate([trig_v[0]] * GQ, axis=0)
        sn = jnp.concatenate([trig_v[1]] * GQ, axis=0)
        prev = rms_rope(q, qg, cs, sn).astype(BF)
        if g:
            at_copy(g - 1).start()
    attend(3, prev)
    at_copy(3).start()

    yn = None
    for g in range(NKV):
        wo_copy(g).wait()
        at_copy(g).wait()
        if g < 2:
            we_c[g + 1].start()
        part = jnp.dot(at_v[g], wo_v[g], preferred_element_type=F32)
        yn = part if g == 0 else yn + part
    yh_v[half] = yn[0:S]
    yp_v[...] = yn[S:2 * S]
    ycp = pltpu.make_async_remote_copy(yp_v, yh_v.at[half], ys_sem, yr_sem, device_id={"ep": mate}, device_id_type=MESH)
    ycp.start()

    mc, mx, my, mz = me % 2, me // 2 % 4, me // 8 % 4, me // 32

    def expert_at(slot):
        i, b, a = (slot >> 1) & 7, (slot >> 4) & 3, slot >> 6
        return (((((mz + a + i) & 3) * 4 + ((my + b + (i >> 1)) & 3)) * 4 + ((mx + (i >> 1)) & 3)) * 2 + ((mc + i) & 1))
    slot = lax.broadcasted_iota(jnp.int32, (CAP * N, S), 0)
    e_col = expert_at(slot)
    ids = ids_v[...]
    chosen = jnp.zeros((CAP * N, S), F32)
    for k in range(8):
        chosen = chosen + jnp.where(ids[k:k + 1, :] == e_col, 1.0, 0.0)
    tri = jnp.where(lax.broadcasted_iota(jnp.int32, (S, S), 0) < lax.broadcasted_iota(jnp.int32, (S, S), 1), 1.0, 0.0)
    rank = jnp.dot(chosen.astype(BF), tri.astype(BF), preferred_element_type=F32)
    send = chosen * jnp.where(rank == (slot & 1).astype(F32), 1.0, 0.0)
    snd_v[...] = jnp.transpose(send)
    p_v[...] = send.astype(BF)

    ycp.wait()
    y = h_v[...].astype(F32) + jnp.concatenate([yh_v[0], yh_v[1]], axis=1)
    y_v[...] = y
    rs = lax.rsqrt(jnp.mean(y * y, axis=-1, keepdims=True) + EPS)
    lnm = lnm_v[...].astype(F32)
    for j in range(16):
        sl = slice(j * 128, (j + 1) * 128)
        r_v[:, sl] = (y[:, sl] * rs * lnm[j:j + 1, :]).astype(BF)

    sview, rview = sbuf.reshape(16, CAP * N, HD), rbuf.reshape(16, CAP * N, HD)
    oview, bview = obuf.reshape(16, CAP * N, HD), bbuf.reshape(16, CAP * N, HD)
    for n in range(4):
        rows = jnp.dot(p_v[...], r_v[:, n * 512:(n + 1) * 512], preferred_element_type=F32).astype(BF)
        for j in range(4):
            sview[n * 4 + j] = rows[:, j * 128:(j + 1) * 128]
    gsz = N // GRP

    def push(src, dst, s_sem, r_sem, t, sign):
        for i, to in enumerate(peers(me, t, sign)):
            if not (isinstance(t, int) and t * 8 + i == 0):
                k = t * 8 + i
                pltpu.make_async_remote_copy(src.at[:, k], dst.at[:, k], s_sem, r_sem, device_id={"ep": to}, device_id_type=MESH).start()

    def push_group(src, dst, s_sem, r_sem, q, sign):
        if q == 0:
            push(src, dst, s_sem, r_sem, 0, sign)

        @pl.loop(max(1, q * gsz // 8), (q + 1) * gsz // 8)
        def _(t):
            push(src, dst, s_sem, r_sem, t, sign)
    for q in range(GRP):
        push_group(sbuf, rbuf, ssem, rsem.at[q], q, 1)
    rbuf[:, 0] = sbuf[:, 0]

    wr_c.wait()
    logits = jnp.dot(r_v[...], wr_v[...], preferred_element_type=F32)
    e2 = expert_at(lax.broadcasted_iota(jnp.int32, (N, CAP * N), 1))
    expand = jnp.where(lax.broadcasted_iota(jnp.int32, (N, CAP * N), 0) == e2, 1.0, 0.0)
    lg = jnp.dot(logits, expand, precision=lax.Precision.HIGHEST, preferred_element_type=F32)
    on = snd_v[...] > 0.5
    top = jnp.max(jnp.where(on, lg, -jnp.inf), axis=-1, keepdims=True)
    ex = jnp.where(on, jnp.exp(jnp.where(on, lg - top, 0.0)), 0.0)
    gates = ex / jnp.sum(ex, axis=-1, keepdims=True)
    g1 = gates.astype(BF)
    d1 = gates - g1.astype(F32)
    g2 = d1.astype(BF)
    g3 = (d1 - g2.astype(F32)).astype(BF)
    g_v[...] = jnp.concatenate([g1, g2, g3], axis=0)
    for c in we_c:
        c.wait()

    rr = CAP * gsz
    for q in range(GRP):
        lo = 1 if q == 0 else q * gsz
        got = rbuf.at[:, pl.ds(lo, (q + 1) * gsz - lo)]
        cp(got, got, rsem.at[q]).wait()

        for n in range(FF // 256):
            cols = slice(n * 256, (n + 1) * 256)
            ga = jnp.zeros((rr, 256), F32)
            ua = jnp.zeros((rr, 256), F32)
            for kk in range(8):
                xk = jnp.concatenate([rview[2 * kk, q * rr:(q + 1) * rr, :], rview[2 * kk + 1, q * rr:(q + 1) * rr, :]], axis=1)
                ga = ga + jnp.dot(xk, wg_v[kk * 256:(kk + 1) * 256, cols], preferred_element_type=F32)
                ua = ua + jnp.dot(xk, wu_v[kk * 256:(kk + 1) * 256, cols], preferred_element_type=F32)
            hid_v[q * rr:(q + 1) * rr, cols] = (jax.nn.silu(ga) * ua).astype(BF)

        for n in range(4):
            cols = slice(n * 512, (n + 1) * 512)
            o = jnp.dot(hid_v[q * rr:(q + 1) * rr, :], wd_v[:, cols], preferred_element_type=F32).astype(BF)
            for j in range(4):
                oview[n * 4 + j, q * rr:(q + 1) * rr, :] = o[:, j * 128:(j + 1) * 128]

        push_group(obuf, bbuf, osem, bsem, q, -1)
    bbuf[:, 0] = obuf[:, 0]

    got = bbuf.at[:, pl.ds(1, N - 1)]
    cp(got, got, bsem).wait()
    for n in range(4):
        back = jnp.concatenate([bview[n * 4 + j] for j in range(4)], axis=1)
        m = jnp.dot(g_v[...], back, preferred_element_type=F32)
        cols = slice(n * 512, (n + 1) * 512)
        out_ref[:, cols] = (y_v[:, cols] + (m[0:S] + m[S:2 * S] + m[2 * S:3 * S])).astype(BF)
    sent = sbuf.at[:, pl.ds(1, N - 1)]
    cp(sent, sent, ssem).wait()
    cp(sent, sent, osem).wait()


def finish(out_hbm, fresh_hbm, kc_hbm, vc_hbm, sl_hbm, res_hbm, ko_hbm, vo_hbm, out_v, fresh_v, c_v, sl_s, sm_in, sm_c, sm_res, sm_o):
    cp = pltpu.make_async_copy
    step = S // FIN
    ins = [cp(sl_hbm, sl_s, sm_in.at[0]), cp(fresh_hbm, fresh_v, sm_in.at[1]), cp(out_hbm, out_v, sm_in.at[2])]
    parts = [(i, p) for p in range(FIN) for i in range(2)]
    cin = {(i, p): cp((kc_hbm, vc_hbm)[i].at[pl.ds(p * step, step)], c_v.at[i, pl.ds(p * step, step)], sm_c.at[i, p]) for i, p in parts}
    cout = {(i, p): cp(c_v.at[i, pl.ds(p * step, step)], (ko_hbm, vo_hbm)[i].at[pl.ds(p * step, step)], sm_o.at[i, p]) for i, p in parts}
    for c in ins:
        c.start()
    for key in parts:
        cin[key].start()
    ins[2].wait()
    res = cp(out_v, res_hbm, sm_res)
    res.start()
    ins[0].wait()
    ins[1].wait()
    trow = lax.broadcasted_iota(jnp.int32, (128, HD), 0) >> 2
    rows = c_v.reshape(2, S * T * NKV, HD)
    for i, p in parts:
        cin[i, p].wait()
        for s in range(p * step, (p + 1) * step):
            old = rows[i, s * 128:(s + 1) * 128, :].astype(F32)
            new = jnp.concatenate([fresh_v[i, s * 16:(s + 1) * 16, :].astype(F32)] * 8, axis=0)
            rows[i, s * 128:(s + 1) * 128, :] = jnp.where(trow == sl_s[s], new, old).astype(BF)
        cout[i, p].start()
    res.wait()
    for key in parts:
        cout[key].wait()


def solution(mesh):
    row_spec = P(('dp', 'ep'), None)
    cache_spec = P(('dp', 'ep'), None, None, None)
    len_spec = P(('dp', 'ep'))
    rep_vec = P(None)
    rep_mat = P(None, None)
    exp_spec = P('ep', None, None)
    inv = np.power(ROPE_BASE, -np.arange(0, HD, 2).astype(np.float32) / HD).astype(np.float32)
    freq_np = np.concatenate([inv, inv])[None, :]
    dma = pltpu.SemaphoreType.DMA

    def local_step(hidden, k_cache, v_cache, seq_lens, expert_ids, ln_attn, w_q, w_k, w_v, q_gain, k_gain, w_o, ln_moe, w_router, w_gate, w_up, w_down):
        anyspec = pl.BlockSpec(memory_space=pl.ANY)
        V = pltpu.VMEM
        out, fresh = pl.pallas_call(
            kernel,
            out_shape=(jax.ShapeDtypeStruct((S, D), BF), jax.ShapeDtypeStruct((2, 256, HD), BF)),
            in_specs=[anyspec] * 18,
            out_specs=(pl.BlockSpec(memory_space=pltpu.VMEM),) * 2,
            scratch_shapes=[
                V((S, D), BF), pltpu.SMEM((S,), jnp.int32), V((8, S), jnp.int32), V((16, 128), BF), V((16, 128), BF),
                V((1, HD), BF), V((1, HD), BF), V((1, HD), F32),
                V((D, 512), BF), V((D, 512), BF), V((4, D, 1024), BF), V((4, 1024, 1024), BF), V((D, N), BF),
                V((D, FF), BF), V((D, FF), BF), V((FF, D), BF),
                V((S, T, NKV, HD), BF), V((S, T, NKV, HD), BF), V((NKV, S * T, HD), BF), V((NKV, S * T, HD), BF),
                V((S, D), BF), V((2, NKV, S, HD), F32), V((S, S * T), F32), V((2, S, HD), F32), V((NKV, 2 * S, 1024), BF), V((2, S, 1024), F32), V((S, 1024), F32),
                V((S, D), F32), V((S, D), BF), V((CAP * N, S), BF), V((S, CAP * N), F32), V((3 * S, CAP * N), BF),
                V((CAP * N, FF), BF),
                V((16, N, CAP, HD), BF), V((16, N, CAP, HD), BF), V((16, N, CAP, HD), BF), V((16, N, CAP, HD), BF),
                dma((8,)), dma((2,)), dma((2,)), dma((4,)), dma((4,)), dma, dma((3,)), dma((4,)), dma((4,)), dma, dma,
                dma, dma, dma((GRP,)), dma,
            ],
            compiler_params=pltpu.CompilerParams(collective_id=0, has_side_effects=True, vmem_limit_bytes=67043328),
        )(hidden, k_cache, v_cache, seq_lens, expert_ids.T, ln_attn.reshape(16, 128), w_q, w_k, w_v,
          q_gain.reshape(1, HD), k_gain.reshape(1, HD), w_o, ln_moe.reshape(16, 128), w_router, w_gate, w_up, w_down,
          jnp.asarray(freq_np))
        return pl.pallas_call(
            finish,
            out_shape=(jax.ShapeDtypeStruct((S, D), BF),
                       jax.ShapeDtypeStruct((S, T, NKV, HD), BF), jax.ShapeDtypeStruct((S, T, NKV, HD), BF)),
            in_specs=[anyspec] * 5,
            out_specs=(anyspec,) * 3,
            scratch_shapes=[V((S, D), BF), V((2, 256, HD), BF), V((2, S, T, NKV, HD), BF), pltpu.SMEM((S,), jnp.int32),
                            dma((3,)), dma((2, FIN)), dma, dma((2, FIN))],
        )(out, fresh, k_cache, v_cache, seq_lens)

    return jax.shard_map(local_step, mesh=mesh, in_specs=(row_spec, cache_spec, cache_spec, len_spec, row_spec, rep_vec, rep_mat, rep_mat, rep_mat, rep_vec, rep_vec, rep_mat, rep_vec, rep_mat, exp_spec, exp_spec, exp_spec), out_specs=(row_spec, cache_spec, cache_spec), check_vma=False)
```

```python
import functools

import jax
import jax.numpy as jnp
import numpy as np
from jax import lax
from jax.experimental import pallas as pl
from jax.experimental.pallas import tpu as pltpu
from jax.sharding import PartitionSpec as P

MESH = pl.DeviceIdType.MESH
EPS = 1e-6
ROPE_BASE = 1000000.0
BF = jnp.bfloat16
F32 = jnp.float32
N = 128
S = 16
D = 2048
HD = 128
T = 32
NKV = 4
GQ = 8
FF = 768
CAP = 2
GROUPS = ((0, 8), (8, 16))
GRP = len(GROUPS)
MUL = 91
STEP = 11


def peers(me, t, sign):
    c, x, y, z = lax.rem(me, 2), lax.rem(lax.div(me, 2), 4), lax.rem(lax.div(me, 8), 4), lax.div(me, 32)
    u = lax.rem(t * STEP, 16)
    a, b = lax.div(u, 4), lax.rem(u, 4)
    zs = [lax.rem(z + 8 + sign * (a + f), 4) * 32 for f in range(4)]
    ys = [lax.rem(y + 8 + sign * (b + g), 4) * 8 for g in range(4)]
    xs = [[lax.rem(x + 4 + sign * d, 4) * 2 + e for e in (c, 1 - c)] for d in range(4)]
    offs = [i * MUL % N for i in range(8)]
    return [zs[o // 32] + ys[o // 8 % 4] + xs[o // 2 % 4][o % 2] for o in offs]


def rms_rope(v, gain, cos, sin):
    ms = jnp.mean(v * v, axis=-1, keepdims=True)
    v = v * lax.rsqrt(ms + EPS) * gain
    return v * cos + pltpu.roll(v, 64, axis=1) * sin


def kernel(h_hbm, kc_hbm, vc_hbm, sl_hbm, ids_hbm, lna_hbm, wq_hbm, wk_hbm, wv_hbm, qg_hbm, kg_hbm, wo_hbm,
           lnm_hbm, wr_hbm, wg_hbm, wu_hbm, wd_hbm, freq_hbm,
           out_ref, kc_v, vc_v,
           h_v, sl_s, ids_v, lna_v, lnm_v, qg_v, kg_v, freq_v,
           wk_v, wv_v, wq_v, wo_v, wr_v, wg_v, wu_v, wd_v,
           kp_v, vp_v, x_v, kn_v, mask_v, trig_v, at_v, yh_v, yp_v, y_v, r_v, p_v, snd_v, g_v, hid_v,
           sbuf, rbuf, obuf, bbuf,
           sm_small, sm_kv, sm_cache, sm_wq, sm_wo, sm_wr, sm_we, as_sem, ar_sem, ys_sem, yr_sem,
           ssem, osem, rsem, bsem):
    me = lax.axis_index("ep")
    cp = pltpu.make_async_copy
    half = me % 2
    mate = me + 1 - 2 * half

    small = [cp(a, b, sm_small.at[i]) for i, (a, b) in enumerate([
        (h_hbm, h_v), (lna_hbm, lna_v), (sl_hbm, sl_s), (freq_hbm, freq_v), (kg_hbm, kg_v), (qg_hbm, qg_v),
        (ids_hbm, ids_v), (lnm_hbm, lnm_v)])]
    for c in small:
        c.start()
    kvw = [cp(wk_hbm, wk_v, sm_kv.at[0]), cp(wv_hbm, wv_v, sm_kv.at[1])]
    caches = [cp(kc_hbm, kc_v, sm_cache.at[0]), cp(vc_hbm, vc_v, sm_cache.at[1])]

    def wq_copy(g):
        return cp(wq_hbm.at[:, pl.ds(pl.multiple_of(g * 1024, 1024), 1024)], wq_v.at[g], sm_wq.at[g])

    def wo_copy(n):
        return cp(wo_hbm.at[pl.ds(n * 1024, 1024), pl.ds(pl.multiple_of(half * 1024, 1024), 1024)], wo_v.at[n], sm_wo.at[n])

    wr_c = cp(wr_hbm, wr_v, sm_wr)
    we_c = [cp(wg_hbm.at[0], wg_v, sm_we.at[0]), cp(wu_hbm.at[0], wu_v, sm_we.at[1]), cp(wd_hbm.at[0], wd_v, sm_we.at[2])]
    for c in kvw + caches:
        c.start()
    wq_copy(0).start()

    bar = pltpu.get_barrier_semaphore()

    for i in range(8):
        pl.semaphore_signal(bar, inc=1, device_id={"ep": lax.rem(me + (i + 1), N)}, device_id_type=MESH)

    @pl.loop(0, 7)
    def _(b):
        base = me + b * 17
        for i in range(17):
            pl.semaphore_signal(bar, inc=1, device_id={"ep": lax.rem(base + (i + 9), N)}, device_id_type=MESH)

    for c in small:
        c.wait()

    wq_copy(1).start()
    wq_copy(2).start()

    hf = h_v[...].astype(F32)
    rs = lax.rsqrt(jnp.mean(hf * hf, axis=-1, keepdims=True) + EPS)
    lna = lna_v[...].astype(F32)
    for j in range(16):
        sl = slice(j * 128, (j + 1) * 128)
        x_v[:, sl] = (hf[:, sl] * rs * lna[j:j + 1, :]).astype(BF)

    srow = lax.broadcasted_iota(jnp.int32, (S, 128), 0)
    lens = jnp.zeros((S, 128), jnp.int32)
    for s in range(S):
        lens = jnp.where(srow == s, sl_s[s], lens)
    ang = lens.astype(F32) * freq_v[...]
    sgn = jnp.where(lax.broadcasted_iota(jnp.int32, (S, 128), 1) < 64, -1.0, 1.0)
    cos = jnp.cos(ang)
    sin = jnp.sin(ang) * sgn
    trig_v[0] = cos
    trig_v[1] = sin
    for b in range(4):
        col = lax.broadcasted_iota(jnp.int32, (S, 128), 1) + b * 128
        ok = ((col >> 5) == srow) & ((col & 31) <= lens)
        mask_v[:, b * 128:(b + 1) * 128] = jnp.where(ok, 0.0, -1e30)

    x = x_v[...]
    kg = kg_v[...].astype(F32)
    kvw[0].wait()
    kp = jnp.dot(x, wk_v[...], preferred_element_type=F32)
    for g in range(NKV):
        kn_v[0, g] = rms_rope(kp[:, g * 128:(g + 1) * 128], kg, cos, sin)
    kvw[1].wait()
    vp = jnp.dot(x, wv_v[...], preferred_element_type=F32)
    for g in range(NKV):
        kn_v[1, g] = vp[:, g * 128:(g + 1) * 128]

    wq_copy(3).start()

    ri = lax.broadcasted_iota(jnp.int32, (256, 64), 0)
    ci = lax.broadcasted_iota(jnp.int32, (256, 64), 1)
    rep1 = jnp.where(((ri >> 4) == (ci & 15)) & ((ri & 3) == (ci >> 4)), 1.0, 0.0).astype(BF)
    pr = lax.broadcasted_iota(jnp.int32, (128, 128), 0)
    pc = lax.broadcasted_iota(jnp.int32, (128, 128), 1)
    perm = jnp.where(((pr & 31) == (pc >> 2)) & ((pr >> 5) == (pc & 3)), 1.0, 0.0).astype(BF)
    trow = pr >> 2
    for i, (buf, dst) in enumerate(((kc_v, kp_v), (vc_v, vp_v))):
        caches[i].wait()
        rows = buf.reshape(S * T * NKV, HD)
        new = jnp.concatenate([kn_v[i, g].astype(BF) for g in range(NKV)], axis=0)
        rep = jnp.dot(rep1, new, preferred_element_type=F32)
        for s in range(S):
            old = rows[s * 128:(s + 1) * 128, :].astype(F32)
            rep_s = jnp.concatenate([rep[s * 16:(s + 1) * 16, :]] * 8, axis=0)
            upd = jnp.where(trow == sl_s[s], rep_s, old).astype(BF)
            rows[s * 128:(s + 1) * 128, :] = upd
            grp = jnp.dot(perm, upd, preferred_element_type=F32).astype(BF)
            for g in range(NKV):
                dst[g, s * 32:(s + 1) * 32, :] = grp[g * 32:(g + 1) * 32, :]

    def at_copy(g):
        return pltpu.make_async_remote_copy(at_v.at[g, pl.ds(0, S)], at_v.at[g, pl.ds(S, S)], as_sem.at[g], ar_sem.at[g],
                                            device_id={"ep": mate}, device_id_type=MESH)

    qg = qg_v[...].astype(F32)

    def attend(g, q):
        sc = lax.dot_general(q, kp_v[g], (((1,), (1,)), ((), ())), preferred_element_type=F32)
        mk = mask_v[...]
        sc = jnp.where(jnp.concatenate([mk] * GQ, axis=0) == 0.0, sc * (HD ** -0.5), -1e30)
        ex = jnp.exp(sc - jnp.max(sc, axis=-1, keepdims=True))
        pb = (ex / jnp.sum(ex, axis=-1, keepdims=True)).astype(BF)
        o = jnp.dot(pb, vp_v[g], preferred_element_type=F32).astype(BF)
        for j in range(GQ):
            at_v[g, 0:S, j * 128:(j + 1) * 128] = o[j * S:(j + 1) * S, :]

    prev = None
    for g in range(NKV):
        wq_copy(g).wait()
        if g == 0:
            wo_copy(0).start()
            wo_copy(1).start()
        elif g < 3:
            wo_copy(g + 1).start()
        else:
            wr_c.start()
            we_c[0].start()
        q = jnp.dot(x_v[...], wq_v[g], preferred_element_type=F32)
        if g:
            attend(g - 1, prev)
        q = jnp.concatenate([q[:, j * 128:(j + 1) * 128] for j in range(GQ)], axis=0)
        cs = jnp.concatenate([trig_v[0]] * GQ, axis=0)
        sn = jnp.concatenate([trig_v[1]] * GQ, axis=0)
        prev = rms_rope(q, qg, cs, sn).astype(BF)
        if g == 1:
            pl.semaphore_wait(bar, N - 1)
        if g:
            at_copy(g - 1).start()
    attend(3, prev)
    at_copy(3).start()

    yn = None
    for g in range(NKV):
        wo_copy(g).wait()
        at_copy(g).wait()
        if g < 2:
            we_c[g + 1].start()
        part = jnp.dot(at_v[g], wo_v[g], preferred_element_type=F32)
        yn = part if g == 0 else yn + part
    yh_v[half] = yn[0:S]
    yp_v[...] = yn[S:2 * S]
    ycp = pltpu.make_async_remote_copy(yp_v, yh_v.at[half], ys_sem, yr_sem, device_id={"ep": mate}, device_id_type=MESH)
    ycp.start()

    mc, mx, my, mz = me % 2, me // 2 % 4, me // 8 % 4, me // 32

    def expert_at(slot):
        o, u = (((slot >> 1) & 7) * MUL) & (N - 1), (slot >> 4) * STEP
        return (((((mz + (u >> 2) + (o >> 5)) & 3) * 4 + ((my + u + (o >> 3)) & 3)) * 4 + ((mx + (o >> 1)) & 3)) * 2
                + ((mc + o) & 1))
    slot = lax.broadcasted_iota(jnp.int32, (CAP * N, S), 0)
    e_col = expert_at(slot)
    ids = ids_v[...]
    chosen = jnp.zeros((CAP * N, S), F32)
    for k in range(8):
        chosen = chosen + jnp.where(ids[k:k + 1, :] == e_col, 1.0, 0.0)
    tri = jnp.where(lax.broadcasted_iota(jnp.int32, (S, S), 0) < lax.broadcasted_iota(jnp.int32, (S, S), 1), 1.0, 0.0)
    rank = jnp.dot(chosen.astype(BF), tri.astype(BF), preferred_element_type=F32)
    send = chosen * jnp.where(rank == (slot & 1).astype(F32), 1.0, 0.0)
    snd_v[...] = jnp.transpose(send)
    p_v[...] = send.astype(BF)

    ycp.wait()
    y = h_v[...].astype(F32) + jnp.concatenate([yh_v[0], yh_v[1]], axis=1)
    y_v[...] = y
    rs = lax.rsqrt(jnp.mean(y * y, axis=-1, keepdims=True) + EPS)
    lnm = lnm_v[...].astype(F32)
    for j in range(16):
        sl = slice(j * 128, (j + 1) * 128)
        r_v[:, sl] = (y[:, sl] * rs * lnm[j:j + 1, :]).astype(BF)

    sview, rview = sbuf.reshape(16, CAP * N, HD), rbuf.reshape(16, CAP * N, HD)
    oview, bview = obuf.reshape(16, CAP * N, HD), bbuf.reshape(16, CAP * N, HD)

    def push(src, dst, s_sem, r_sem, t, sign):
        for i, to in enumerate(peers(me, t, sign)):
            if not (isinstance(t, int) and t * 8 + i == 0):
                k = t * 8 + i
                pltpu.make_async_remote_copy(src.at[:, k], dst.at[:, k], s_sem, r_sem, device_id={"ep": to}, device_id_type=MESH).start()

    def push_group(src, dst, s_sem, r_sem, q, sign):
        if GROUPS[q][0] == 0:
            push(src, dst, s_sem, r_sem, 0, sign)

        @pl.loop(max(1, GROUPS[q][0]), GROUPS[q][1])
        def _(t):
            push(src, dst, s_sem, r_sem, t, sign)
    for q in range(GRP):
        r0, r1 = GROUPS[q][0] * 8 * CAP, GROUPS[q][1] * 8 * CAP
        for n in range(4):
            rows = jnp.dot(p_v[r0:r1, :], r_v[:, n * 512:(n + 1) * 512], preferred_element_type=F32).astype(BF)
            for j in range(4):
                sview[n * 4 + j, r0:r1, :] = rows[:, j * 128:(j + 1) * 128]
        push_group(sbuf, rbuf, ssem, rsem.at[q], q, 1)
    rbuf[:, 0] = sbuf[:, 0]

    wr_c.wait()
    logits = jnp.dot(r_v[...], wr_v[...], preferred_element_type=F32)
    e2 = expert_at(lax.broadcasted_iota(jnp.int32, (N, CAP * N), 1))
    expand = jnp.where(lax.broadcasted_iota(jnp.int32, (N, CAP * N), 0) == e2, 1.0, 0.0)
    lg = jnp.dot(logits, expand, precision=lax.Precision.HIGHEST, preferred_element_type=F32)
    on = snd_v[...] > 0.5
    top = jnp.max(jnp.where(on, lg, -jnp.inf), axis=-1, keepdims=True)
    ex = jnp.where(on, jnp.exp(jnp.where(on, lg - top, 0.0)), 0.0)
    gates = ex / jnp.sum(ex, axis=-1, keepdims=True)
    g1 = gates.astype(BF)
    d1 = gates - g1.astype(F32)
    g2 = d1.astype(BF)
    g3 = (d1 - g2.astype(F32)).astype(BF)
    g_v[...] = jnp.concatenate([g1, g2, g3], axis=0)
    for c in we_c:
        c.wait()

    for q in range(GRP):
        lo, hi = max(1, GROUPS[q][0] * 8), GROUPS[q][1] * 8
        r0, r1 = GROUPS[q][0] * 8 * CAP, hi * CAP
        got = rbuf.at[:, pl.ds(lo, hi - lo)]
        cp(got, got, rsem.at[q]).wait()

        for n in range(FF // 256):
            cols = slice(n * 256, (n + 1) * 256)
            ga = jnp.zeros((r1 - r0, 256), F32)
            ua = jnp.zeros((r1 - r0, 256), F32)
            for kk in range(8):
                xk = jnp.concatenate([rview[2 * kk, r0:r1, :], rview[2 * kk + 1, r0:r1, :]], axis=1)
                ga = ga + jnp.dot(xk, wg_v[kk * 256:(kk + 1) * 256, cols], preferred_element_type=F32)
                ua = ua + jnp.dot(xk, wu_v[kk * 256:(kk + 1) * 256, cols], preferred_element_type=F32)
            hid_v[r0:r1, cols] = (jax.nn.silu(ga) * ua).astype(BF)

        for n in range(4):
            cols = slice(n * 512, (n + 1) * 512)
            o = jnp.dot(hid_v[r0:r1, :], wd_v[:, cols], preferred_element_type=F32).astype(BF)
            for j in range(4):
                oview[n * 4 + j, r0:r1, :] = o[:, j * 128:(j + 1) * 128]

        push_group(obuf, bbuf, osem, bsem, q, -1)
    bbuf[:, 0] = obuf[:, 0]

    got = bbuf.at[:, pl.ds(1, N - 1)]
    cp(got, got, bsem).wait()
    for n in range(4):
        back = jnp.concatenate([bview[n * 4 + j] for j in range(4)], axis=1)
        m = jnp.dot(g_v[...], back, preferred_element_type=F32)
        cols = slice(n * 512, (n + 1) * 512)
        out_ref[:, cols] = (y_v[:, cols] + (m[0:S] + m[S:2 * S] + m[2 * S:3 * S])).astype(BF)
    sent = sbuf.at[:, pl.ds(1, N - 1)]
    cp(sent, sent, ssem).wait()
    cp(sent, sent, osem).wait()


def finish(a_ref, b_ref, c_ref, a_out, b_out, c_out, sems):
    copies = [pltpu.make_async_copy(x, y, sems.at[i]) for i, (x, y) in enumerate(((a_ref, a_out), (b_ref, b_out), (c_ref, c_out)))]
    for c in copies:
        c.start()
    for c in copies:
        c.wait()


def solution(mesh):
    row_spec = P(('dp', 'ep'), None)
    cache_spec = P(('dp', 'ep'), None, None, None)
    len_spec = P(('dp', 'ep'))
    rep_vec = P(None)
    rep_mat = P(None, None)
    exp_spec = P('ep', None, None)
    inv = np.power(ROPE_BASE, -np.arange(0, HD, 2).astype(np.float32) / HD).astype(np.float32)
    freq_np = np.concatenate([inv, inv])[None, :]
    dma = pltpu.SemaphoreType.DMA

    def local_step(hidden, k_cache, v_cache, seq_lens, expert_ids, ln_attn, w_q, w_k, w_v, q_gain, k_gain, w_o, ln_moe, w_router, w_gate, w_up, w_down):
        anyspec = pl.BlockSpec(memory_space=pl.ANY)
        V = pltpu.VMEM
        made = pl.pallas_call(
            kernel,
            out_shape=(V((S, D), BF), V((S, T, NKV, HD), BF), V((S, T, NKV, HD), BF)),
            in_specs=[anyspec] * 18,
            out_specs=(pl.BlockSpec(memory_space=pltpu.VMEM),) * 3,
            scratch_shapes=[
                V((S, D), BF), pltpu.SMEM((S,), jnp.int32), V((8, S), jnp.int32), V((16, 128), BF), V((16, 128), BF),
                V((1, HD), BF), V((1, HD), BF), V((1, HD), F32),
                V((D, 512), BF), V((D, 512), BF), V((4, D, 1024), BF), V((4, 1024, 1024), BF), V((D, N), BF),
                V((D, FF), BF), V((D, FF), BF), V((FF, D), BF),
                V((NKV, S * T, HD), BF), V((NKV, S * T, HD), BF),
                V((S, D), BF), V((2, NKV, S, HD), F32), V((S, S * T), F32), V((2, S, HD), F32), V((NKV, 2 * S, 1024), BF), V((2, S, 1024), F32), V((S, 1024), F32),
                V((S, D), F32), V((S, D), BF), V((CAP * N, S), BF), V((S, CAP * N), F32), V((3 * S, CAP * N), BF),
                V((CAP * N, FF), BF),
                V((16, N, CAP, HD), BF), V((16, N, CAP, HD), BF), V((16, N, CAP, HD), BF), V((16, N, CAP, HD), BF),
                dma((8,)), dma((2,)), dma((2,)), dma((4,)), dma((4,)), dma, dma((3,)), dma((4,)), dma((4,)), dma, dma,
                dma, dma, dma((GRP,)), dma,
            ],
            compiler_params=pltpu.CompilerParams(collective_id=0, has_side_effects=True, vmem_limit_bytes=60 * 1024 * 1024),
        )(hidden, k_cache, v_cache, seq_lens, expert_ids.T, ln_attn.reshape(16, 128), w_q, w_k, w_v,
          q_gain.reshape(1, HD), k_gain.reshape(1, HD), w_o, ln_moe.reshape(16, 128), w_router, w_gate, w_up, w_down,
          jnp.asarray(freq_np))
        return pl.pallas_call(
            finish,
            out_shape=(jax.ShapeDtypeStruct((S, D), BF),
                       jax.ShapeDtypeStruct((S, T, NKV, HD), BF), jax.ShapeDtypeStruct((S, T, NKV, HD), BF)),
            in_specs=[pl.BlockSpec(memory_space=pltpu.VMEM)] * 3,
            out_specs=(anyspec,) * 3,
            scratch_shapes=[dma((3,))],
        )(*[pltpu.with_memory_space_constraint(m, pltpu.VMEM) for m in made])

    return jax.shard_map(local_step, mesh=mesh, in_specs=(row_spec, cache_spec, cache_spec, len_spec, row_spec, rep_vec, rep_mat, rep_mat, rep_mat, rep_vec, rep_vec, rep_mat, rep_vec, rep_mat, exp_spec, exp_spec, exp_spec), out_specs=(row_spec, cache_spec, cache_spec), check_vma=False)
```

```python
import functools

import jax
import jax.numpy as jnp
import numpy as np
from jax import lax
from jax.experimental import pallas as pl
from jax.experimental.pallas import tpu as pltpu
from jax.sharding import PartitionSpec as P

MESH = pl.DeviceIdType.MESH
EPS = 1e-6
ROPE_BASE = 1000000.0
BF = jnp.bfloat16
F32 = jnp.float32
N = 128
S = 16
D = 2048
HD = 128
T = 32
NKV = 4
GQ = 8
FF = 768
CAP = 2
GROUPS = ((0, 4), (4, 8), (8, 12), (12, 16))
GRP = len(GROUPS)
MUL = 91
STEP = 11


def peers(me, t, sign):
    c, x, y, z = lax.rem(me, 2), lax.rem(lax.div(me, 2), 4), lax.rem(lax.div(me, 8), 4), lax.div(me, 32)
    u = lax.rem(t * STEP, 16)
    a, b = lax.div(u, 4), lax.rem(u, 4)
    zs = [lax.rem(z + 8 + sign * (a + f), 4) * 32 for f in range(4)]
    ys = [lax.rem(y + 8 + sign * (b + g), 4) * 8 for g in range(4)]
    xs = [[lax.rem(x + 4 + sign * d, 4) * 2 + e for e in (c, 1 - c)] for d in range(4)]
    offs = [i * MUL % N for i in range(8)]
    return [zs[o // 32] + ys[o // 8 % 4] + xs[o // 2 % 4][o % 2] for o in offs]


def rms_rope(v, gain, cos, sin):
    ms = jnp.mean(v * v, axis=-1, keepdims=True)
    v = v * lax.rsqrt(ms + EPS) * gain
    return v * cos + pltpu.roll(v, 64, axis=1) * sin


def kernel(h_hbm, kc_hbm, vc_hbm, sl_hbm, ids_hbm, lna_hbm, wq_hbm, wk_hbm, wv_hbm, qg_hbm, kg_hbm, wo_hbm,
           lnm_hbm, wr_hbm, wg_hbm, wu_hbm, wd_hbm, freq_hbm,
           out_ref, kc_v, vc_v,
           h_v, sl_s, ids_v, lna_v, lnm_v, qg_v, kg_v, freq_v,
           wk_v, wv_v, wq_v, wo_v, wr_v, wg_v, wu_v, wd_v,
           kp_v, vp_v, x_v, kn_v, mask_v, trig_v, at_v, yh_v, yp_v, y_v, r_v, p_v, snd_v, g_v, hid_v,
           sbuf, rbuf, obuf, bbuf,
           sm_small, sm_kv, sm_cache, sm_wq, sm_wo, sm_wr, sm_we, as_sem, ar_sem, ys_sem, yr_sem,
           ssem, osem, rsem, bsem):
    me = lax.axis_index("ep")
    cp = pltpu.make_async_copy
    half = me % 2
    mate = me + 1 - 2 * half

    small = [cp(a, b, sm_small.at[i]) for i, (a, b) in enumerate([
        (h_hbm, h_v), (lna_hbm, lna_v), (sl_hbm, sl_s), (freq_hbm, freq_v), (kg_hbm, kg_v), (qg_hbm, qg_v),
        (ids_hbm, ids_v), (lnm_hbm, lnm_v)])]
    for c in small:
        c.start()
    kvw = [cp(wk_hbm, wk_v, sm_kv.at[0]), cp(wv_hbm, wv_v, sm_kv.at[1])]
    caches = [cp(kc_hbm, kc_v, sm_cache.at[0]), cp(vc_hbm, vc_v, sm_cache.at[1])]

    def wq_copy(g):
        return cp(wq_hbm.at[:, pl.ds(pl.multiple_of(g * 1024, 1024), 1024)], wq_v.at[g], sm_wq.at[g])

    def wo_copy(n):
        return cp(wo_hbm.at[pl.ds(n * 1024, 1024), pl.ds(pl.multiple_of(half * 1024, 1024), 1024)], wo_v.at[n], sm_wo.at[n])

    wr_c = cp(wr_hbm, wr_v, sm_wr)
    we_c = [cp(wg_hbm.at[0], wg_v, sm_we.at[0]), cp(wu_hbm.at[0], wu_v, sm_we.at[1]), cp(wd_hbm.at[0], wd_v, sm_we.at[2])]
    for c in kvw + caches:
        c.start()
    wq_copy(0).start()

    bar = pltpu.get_barrier_semaphore()

    for i in range(8):
        pl.semaphore_signal(bar, inc=1, device_id={"ep": lax.rem(me + (i + 1), N)}, device_id_type=MESH)

    @pl.loop(0, 7)
    def _(b):
        base = me + b * 17
        for i in range(17):
            pl.semaphore_signal(bar, inc=1, device_id={"ep": lax.rem(base + (i + 9), N)}, device_id_type=MESH)

    for c in small:
        c.wait()

    wq_copy(1).start()
    wq_copy(2).start()

    hf = h_v[...].astype(F32)
    rs = lax.rsqrt(jnp.mean(hf * hf, axis=-1, keepdims=True) + EPS)
    lna = lna_v[...].astype(F32)
    for j in range(16):
        sl = slice(j * 128, (j + 1) * 128)
        x_v[:, sl] = (hf[:, sl] * rs * lna[j:j + 1, :]).astype(BF)

    srow = lax.broadcasted_iota(jnp.int32, (S, 128), 0)
    lens = jnp.zeros((S, 128), jnp.int32)
    for s in range(S):
        lens = jnp.where(srow == s, sl_s[s], lens)
    ang = lens.astype(F32) * freq_v[...]
    sgn = jnp.where(lax.broadcasted_iota(jnp.int32, (S, 128), 1) < 64, -1.0, 1.0)
    cos = jnp.cos(ang)
    sin = jnp.sin(ang) * sgn
    trig_v[0] = cos
    trig_v[1] = sin
    for b in range(4):
        col = lax.broadcasted_iota(jnp.int32, (S, 128), 1) + b * 128
        ok = ((col >> 5) == srow) & ((col & 31) <= lens)
        mask_v[:, b * 128:(b + 1) * 128] = jnp.where(ok, 0.0, -1e30)

    x = x_v[...]
    kg = kg_v[...].astype(F32)
    kvw[0].wait()
    kp = jnp.dot(x, wk_v[...], preferred_element_type=F32)
    for g in range(NKV):
        kn_v[0, g] = rms_rope(kp[:, g * 128:(g + 1) * 128], kg, cos, sin)
    kvw[1].wait()
    vp = jnp.dot(x, wv_v[...], preferred_element_type=F32)
    for g in range(NKV):
        kn_v[1, g] = vp[:, g * 128:(g + 1) * 128]

    wq_copy(3).start()

    ri = lax.broadcasted_iota(jnp.int32, (256, 64), 0)
    ci = lax.broadcasted_iota(jnp.int32, (256, 64), 1)
    rep1 = jnp.where(((ri >> 4) == (ci & 15)) & ((ri & 3) == (ci >> 4)), 1.0, 0.0).astype(BF)
    pr = lax.broadcasted_iota(jnp.int32, (128, 128), 0)
    pc = lax.broadcasted_iota(jnp.int32, (128, 128), 1)
    perm = jnp.where(((pr & 31) == (pc >> 2)) & ((pr >> 5) == (pc & 3)), 1.0, 0.0).astype(BF)
    trow = pr >> 2
    for i, (buf, dst) in enumerate(((kc_v, kp_v), (vc_v, vp_v))):
        caches[i].wait()
        rows = buf.reshape(S * T * NKV, HD)
        new = jnp.concatenate([kn_v[i, g].astype(BF) for g in range(NKV)], axis=0)
        rep = jnp.dot(rep1, new, preferred_element_type=F32)
        for s in range(S):
            old = rows[s * 128:(s + 1) * 128, :].astype(F32)
            rep_s = jnp.concatenate([rep[s * 16:(s + 1) * 16, :]] * 8, axis=0)
            upd = jnp.where(trow == sl_s[s], rep_s, old).astype(BF)
            rows[s * 128:(s + 1) * 128, :] = upd
            grp = jnp.dot(perm, upd, preferred_element_type=F32).astype(BF)
            for g in range(NKV):
                dst[g, s * 32:(s + 1) * 32, :] = grp[g * 32:(g + 1) * 32, :]

    def at_copy(g):
        return pltpu.make_async_remote_copy(at_v.at[g, pl.ds(0, S)], at_v.at[g, pl.ds(S, S)], as_sem.at[g], ar_sem.at[g],
                                            device_id={"ep": mate}, device_id_type=MESH)

    qg = qg_v[...].astype(F32)

    def attend(g, q):
        sc = lax.dot_general(q, kp_v[g], (((1,), (1,)), ((), ())), preferred_element_type=F32)
        mk = mask_v[...]
        sc = jnp.where(jnp.concatenate([mk] * GQ, axis=0) == 0.0, sc * (HD ** -0.5), -1e30)
        ex = jnp.exp(sc - jnp.max(sc, axis=-1, keepdims=True))
        pb = (ex / jnp.sum(ex, axis=-1, keepdims=True)).astype(BF)
        o = jnp.dot(pb, vp_v[g], preferred_element_type=F32).astype(BF)
        for j in range(GQ):
            at_v[g, 0:S, j * 128:(j + 1) * 128] = o[j * S:(j + 1) * S, :]

    prev = None
    for g in range(NKV):
        wq_copy(g).wait()
        if g == 0:
            wo_copy(0).start()
            wo_copy(1).start()
        elif g < 3:
            wo_copy(g + 1).start()
        else:
            wr_c.start()
            we_c[0].start()
        q = jnp.dot(x_v[...], wq_v[g], preferred_element_type=F32)
        if g:
            attend(g - 1, prev)
        q = jnp.concatenate([q[:, j * 128:(j + 1) * 128] for j in range(GQ)], axis=0)
        cs = jnp.concatenate([trig_v[0]] * GQ, axis=0)
        sn = jnp.concatenate([trig_v[1]] * GQ, axis=0)
        prev = rms_rope(q, qg, cs, sn).astype(BF)
        if g == 1:
            pl.semaphore_wait(bar, N - 1)
        if g:
            at_copy(g - 1).start()
    wo_copy(0).wait()
    at_copy(0).wait()
    yn = jnp.dot(at_v[0], wo_v[0], preferred_element_type=F32)
    attend(3, prev)
    at_copy(3).start()
    we_c[1].start()

    for g in range(1, NKV):
        wo_copy(g).wait()
        at_copy(g).wait()
        if g == 1:
            we_c[2].start()
        yn = yn + jnp.dot(at_v[g], wo_v[g], preferred_element_type=F32)
    yh_v[half] = yn[0:S]
    yp_v[...] = yn[S:2 * S]
    ycp = pltpu.make_async_remote_copy(yp_v, yh_v.at[half], ys_sem, yr_sem, device_id={"ep": mate}, device_id_type=MESH)
    ycp.start()

    mc, mx, my, mz = me % 2, me // 2 % 4, me // 8 % 4, me // 32

    def expert_at(slot):
        o, u = (((slot >> 1) & 7) * MUL) & (N - 1), (slot >> 4) * STEP
        return (((((mz + (u >> 2) + (o >> 5)) & 3) * 4 + ((my + u + (o >> 3)) & 3)) * 4 + ((mx + (o >> 1)) & 3)) * 2
                + ((mc + o) & 1))
    slot = lax.broadcasted_iota(jnp.int32, (CAP * N, S), 0)
    e_col = expert_at(slot)
    ids = ids_v[...]
    chosen = jnp.zeros((CAP * N, S), F32)
    for k in range(8):
        chosen = chosen + jnp.where(ids[k:k + 1, :] == e_col, 1.0, 0.0)
    tri = jnp.where(lax.broadcasted_iota(jnp.int32, (S, S), 0) < lax.broadcasted_iota(jnp.int32, (S, S), 1), 1.0, 0.0)
    rank = jnp.dot(chosen.astype(BF), tri.astype(BF), preferred_element_type=F32)
    send = chosen * jnp.where(rank == (slot & 1).astype(F32), 1.0, 0.0)
    snd_v[...] = jnp.transpose(send)
    p_v[...] = send.astype(BF)

    ycp.wait()
    y = h_v[...].astype(F32) + jnp.concatenate([yh_v[0], yh_v[1]], axis=1)
    y_v[...] = y
    rs = lax.rsqrt(jnp.mean(y * y, axis=-1, keepdims=True) + EPS)
    lnm = lnm_v[...].astype(F32)
    for j in range(16):
        sl = slice(j * 128, (j + 1) * 128)
        r_v[:, sl] = (y[:, sl] * rs * lnm[j:j + 1, :]).astype(BF)

    sview, rview = sbuf.reshape(16, CAP * N, HD), rbuf.reshape(16, CAP * N, HD)
    oview, bview = obuf.reshape(16, CAP * N, HD), bbuf.reshape(16, CAP * N, HD)

    def push(src, dst, s_sem, r_sem, t, sign):
        for i, to in enumerate(peers(me, t, sign)):
            if not (isinstance(t, int) and t * 8 + i == 0):
                k = t * 8 + i
                pltpu.make_async_remote_copy(src.at[:, k], dst.at[:, k], s_sem, r_sem, device_id={"ep": to}, device_id_type=MESH).start()

    def push_group(src, dst, s_sem, r_sem, q, sign):
        if GROUPS[q][0] == 0:
            push(src, dst, s_sem, r_sem, 0, sign)

        @pl.loop(max(1, GROUPS[q][0]), GROUPS[q][1])
        def _(t):
            push(src, dst, s_sem, r_sem, t, sign)
    for q in range(GRP):
        r0, r1 = GROUPS[q][0] * 8 * CAP, GROUPS[q][1] * 8 * CAP
        for n in range(4):
            rows = jnp.dot(p_v[r0:r1, :], r_v[:, n * 512:(n + 1) * 512], preferred_element_type=F32).astype(BF)
            for j in range(4):
                sview[n * 4 + j, r0:r1, :] = rows[:, j * 128:(j + 1) * 128]
        push_group(sbuf, rbuf, ssem, rsem.at[q], q, 1)
    rbuf[:, 0] = sbuf[:, 0]

    wr_c.wait()
    logits = jnp.dot(r_v[...], wr_v[...], preferred_element_type=F32)
    e2 = expert_at(lax.broadcasted_iota(jnp.int32, (N, CAP * N), 1))
    expand = jnp.where(lax.broadcasted_iota(jnp.int32, (N, CAP * N), 0) == e2, 1.0, 0.0)
    lg = jnp.dot(logits, expand, precision=lax.Precision.HIGHEST, preferred_element_type=F32)
    on = snd_v[...] > 0.5
    top = jnp.max(jnp.where(on, lg, -jnp.inf), axis=-1, keepdims=True)
    ex = jnp.where(on, jnp.exp(jnp.where(on, lg - top, 0.0)), 0.0)
    gates = ex / jnp.sum(ex, axis=-1, keepdims=True)
    g1 = gates.astype(BF)
    d1 = gates - g1.astype(F32)
    g2 = d1.astype(BF)
    g3 = (d1 - g2.astype(F32)).astype(BF)
    g_v[...] = jnp.concatenate([g1, g2, g3], axis=0)
    for c in we_c:
        c.wait()

    for q in range(GRP):
        lo, hi = max(1, GROUPS[q][0] * 8), GROUPS[q][1] * 8
        r0, r1 = GROUPS[q][0] * 8 * CAP, hi * CAP
        got = rbuf.at[:, pl.ds(lo, hi - lo)]
        cp(got, got, rsem.at[q]).wait()

        for n in range(FF // 256):
            cols = slice(n * 256, (n + 1) * 256)
            ga = jnp.zeros((r1 - r0, 256), F32)
            ua = jnp.zeros((r1 - r0, 256), F32)
            for kk in range(8):
                xk = jnp.concatenate([rview[2 * kk, r0:r1, :], rview[2 * kk + 1, r0:r1, :]], axis=1)
                ga = ga + jnp.dot(xk, wg_v[kk * 256:(kk + 1) * 256, cols], preferred_element_type=F32)
                ua = ua + jnp.dot(xk, wu_v[kk * 256:(kk + 1) * 256, cols], preferred_element_type=F32)
            hid_v[r0:r1, cols] = (jax.nn.silu(ga) * ua).astype(BF)

        for n in range(4):
            cols = slice(n * 512, (n + 1) * 512)
            o = jnp.dot(hid_v[r0:r1, :], wd_v[:, cols], preferred_element_type=F32).astype(BF)
            for j in range(4):
                oview[n * 4 + j, r0:r1, :] = o[:, j * 128:(j + 1) * 128]

        push_group(obuf, bbuf, osem, bsem.at[q], q, -1)
        if q == 0:
            bbuf[:, 0] = obuf[:, 0]

    for q in range(GRP):
        lo, hi = max(1, GROUPS[q][0] * 8), GROUPS[q][1] * 8
        r0, r1 = GROUPS[q][0] * 8 * CAP, hi * CAP
        got = bbuf.at[:, pl.ds(lo, hi - lo)]
        cp(got, got, bsem.at[q]).wait()
        for n in range(4):
            back = jnp.concatenate([bview[n * 4 + j, r0:r1, :] for j in range(4)], axis=1)
            m = jnp.dot(g_v[:, r0:r1], back, preferred_element_type=F32)
            cols = slice(n * 512, (n + 1) * 512)
            tot = y_v[:, cols] + (m[0:S] + m[S:2 * S] + m[2 * S:3 * S])
            if q + 1 < GRP:
                y_v[:, cols] = tot
            else:
                out_ref[:, cols] = tot.astype(BF)
    sent = sbuf.at[:, pl.ds(1, N - 1)]
    cp(sent, sent, ssem).wait()
    cp(sent, sent, osem).wait()


def finish(a_ref, b_ref, c_ref, a_out, b_out, c_out, sems):
    copies = [pltpu.make_async_copy(x, y, sems.at[i]) for i, (x, y) in enumerate(((a_ref, a_out), (b_ref, b_out), (c_ref, c_out)))]
    for c in copies:
        c.start()
    for c in copies:
        c.wait()


def solution(mesh):
    row_spec = P(('dp', 'ep'), None)
    cache_spec = P(('dp', 'ep'), None, None, None)
    len_spec = P(('dp', 'ep'))
    rep_vec = P(None)
    rep_mat = P(None, None)
    exp_spec = P('ep', None, None)
    inv = np.power(ROPE_BASE, -np.arange(0, HD, 2).astype(np.float32) / HD).astype(np.float32)
    freq_np = np.concatenate([inv, inv])[None, :]
    dma = pltpu.SemaphoreType.DMA

    def local_step(hidden, k_cache, v_cache, seq_lens, expert_ids, ln_attn, w_q, w_k, w_v, q_gain, k_gain, w_o, ln_moe, w_router, w_gate, w_up, w_down):
        anyspec = pl.BlockSpec(memory_space=pl.ANY)
        V = pltpu.VMEM
        made = pl.pallas_call(
            kernel,
            out_shape=(V((S, D), BF), V((S, T, NKV, HD), BF), V((S, T, NKV, HD), BF)),
            in_specs=[anyspec] * 18,
            out_specs=(pl.BlockSpec(memory_space=pltpu.VMEM),) * 3,
            scratch_shapes=[
                V((S, D), BF), pltpu.SMEM((S,), jnp.int32), V((8, S), jnp.int32), V((16, 128), BF), V((16, 128), BF),
                V((1, HD), BF), V((1, HD), BF), V((1, HD), F32),
                V((D, 512), BF), V((D, 512), BF), V((4, D, 1024), BF), V((4, 1024, 1024), BF), V((D, N), BF),
                V((D, FF), BF), V((D, FF), BF), V((FF, D), BF),
                V((NKV, S * T, HD), BF), V((NKV, S * T, HD), BF),
                V((S, D), BF), V((2, NKV, S, HD), F32), V((S, S * T), F32), V((2, S, HD), F32), V((NKV, 2 * S, 1024), BF), V((2, S, 1024), F32), V((S, 1024), F32),
                V((S, D), F32), V((S, D), BF), V((CAP * N, S), BF), V((S, CAP * N), F32), V((3 * S, CAP * N), BF),
                V((CAP * N, FF), BF),
                V((16, N, CAP, HD), BF), V((16, N, CAP, HD), BF), V((16, N, CAP, HD), BF), V((16, N, CAP, HD), BF),
                dma((8,)), dma((2,)), dma((2,)), dma((4,)), dma((4,)), dma, dma((3,)), dma((4,)), dma((4,)), dma, dma,
                dma, dma, dma((GRP,)), dma((GRP,)),
            ],
            compiler_params=pltpu.CompilerParams(collective_id=0, has_side_effects=True, vmem_limit_bytes=60 * 1024 * 1024),
        )(hidden, k_cache, v_cache, seq_lens, expert_ids.T, ln_attn.reshape(16, 128), w_q, w_k, w_v,
          q_gain.reshape(1, HD), k_gain.reshape(1, HD), w_o, ln_moe.reshape(16, 128), w_router, w_gate, w_up, w_down,
          jnp.asarray(freq_np))
        return pl.pallas_call(
            finish,
            out_shape=(jax.ShapeDtypeStruct((S, D), BF),
                       jax.ShapeDtypeStruct((S, T, NKV, HD), BF), jax.ShapeDtypeStruct((S, T, NKV, HD), BF)),
            in_specs=[pl.BlockSpec(memory_space=pltpu.VMEM)] * 3,
            out_specs=(anyspec,) * 3,
            scratch_shapes=[dma((3,))],
        )(*[pltpu.with_memory_space_constraint(m, pltpu.VMEM) for m in made])

    return jax.shard_map(local_step, mesh=mesh, in_specs=(row_spec, cache_spec, cache_spec, len_spec, row_spec, rep_vec, rep_mat, rep_mat, rep_mat, rep_vec, rep_vec, rep_mat, rep_vec, rep_mat, exp_spec, exp_spec, exp_spec), out_specs=(row_spec, cache_spec, cache_spec), check_vma=False)
```

```python
import functools

import jax
import jax.numpy as jnp
import numpy as np
from jax import lax
from jax.experimental import pallas as pl
from jax.experimental.pallas import tpu as pltpu
from jax.sharding import PartitionSpec as P

MESH = pl.DeviceIdType.MESH
EPS = 1e-6
ROPE_BASE = 1000000.0
BF = jnp.bfloat16
F32 = jnp.float32
N = 128
S = 16
D = 2048
HD = 128
T = 32
NKV = 4
GQ = 8
FF = 768
CAP = 2
GROUPS = ((0, 4), (4, 8), (8, 12), (12, 16))
GRP = len(GROUPS)
MUL = 91
STEP = 11


def peers(me, t, sign):
    c, x, y, z = lax.rem(me, 2), lax.rem(lax.div(me, 2), 4), lax.rem(lax.div(me, 8), 4), lax.div(me, 32)
    u = lax.rem(t * STEP, 16)
    a, b = lax.div(u, 4), lax.rem(u, 4)
    zs = [lax.rem(z + 8 + sign * (a + f), 4) * 32 for f in range(4)]
    ys = [lax.rem(y + 8 + sign * (b + g), 4) * 8 for g in range(4)]
    xs = [[lax.rem(x + 4 + sign * d, 4) * 2 + e for e in (c, 1 - c)] for d in range(4)]
    offs = [i * MUL % N for i in range(8)]
    return [zs[o // 32] + ys[o // 8 % 4] + xs[o // 2 % 4][o % 2] for o in offs]


def rms_rope(v, gain, cos, sin):
    ms = jnp.mean(v * v, axis=-1, keepdims=True)
    v = v * lax.rsqrt(ms + EPS) * gain
    return v * cos + pltpu.roll(v, 64, axis=1) * sin


def kernel(h_hbm, kc_hbm, vc_hbm, sl_hbm, ids_hbm, lna_hbm, wq_hbm, wk_hbm, wv_hbm, qg_hbm, kg_hbm, wo_hbm,
           lnm_hbm, wr_hbm, wg_hbm, wu_hbm, wd_hbm, freq_hbm,
           out_ref, kc_v, vc_v,
           h_v, sl_s, ids_v, lna_v, lnm_v, qg_v, kg_v, freq_v,
           wk_v, wv_v, wq_v, wo_v, wr_v, wg_v, wu_v, wd_v,
           kp_v, vp_v, x_v, kn_v, mask_v, trig_v, at_v, yh_v, yp_v, y_v, r_v, p_v, snd_v, g_v, hid_v,
           sbuf, rbuf, obuf, bbuf,
           sm_small, sm_kv, sm_cache, sm_wq, sm_wo, sm_wr, sm_we, as_sem, ar_sem, ys_sem, yr_sem,
           ssem, osem, rsem, bsem):
    me = lax.axis_index("ep")
    cp = pltpu.make_async_copy
    half = me % 2
    mate = me + 1 - 2 * half

    small = [cp(a, b, sm_small.at[i]) for i, (a, b) in enumerate([
        (h_hbm, h_v), (lna_hbm, lna_v), (sl_hbm, sl_s), (freq_hbm, freq_v), (kg_hbm, kg_v), (qg_hbm, qg_v),
        (ids_hbm, ids_v), (lnm_hbm, lnm_v)])]
    for c in small:
        c.start()
    kvw = [cp(wk_hbm, wk_v, sm_kv.at[0]), cp(wv_hbm, wv_v, sm_kv.at[1])]
    caches = [cp(kc_hbm, kc_v, sm_cache.at[0]), cp(vc_hbm, vc_v, sm_cache.at[1])]

    def wq_copy(g):
        return cp(wq_hbm.at[:, pl.ds(pl.multiple_of(g * 1024, 1024), 1024)], wq_v.at[g], sm_wq.at[g])

    def wo_copy(n):
        return cp(wo_hbm.at[pl.ds(n * 1024, 1024), pl.ds(pl.multiple_of(half * 1024, 1024), 1024)], wo_v.at[n], sm_wo.at[n])

    wr_c = cp(wr_hbm, wr_v, sm_wr)
    we_c = [cp(wg_hbm.at[0], wg_v, sm_we.at[0]), cp(wu_hbm.at[0], wu_v, sm_we.at[1]), cp(wd_hbm.at[0], wd_v, sm_we.at[2])]
    for c in kvw + caches:
        c.start()
    wq_copy(0).start()

    bar = pltpu.get_barrier_semaphore()

    for i in range(8):
        pl.semaphore_signal(bar, inc=1, device_id={"ep": lax.rem(me + (i + 1), N)}, device_id_type=MESH)

    @pl.loop(0, 7)
    def _(b):
        base = me + b * 17
        for i in range(17):
            pl.semaphore_signal(bar, inc=1, device_id={"ep": lax.rem(base + (i + 9), N)}, device_id_type=MESH)

    for c in small:
        c.wait()

    wq_copy(1).start()
    wq_copy(2).start()

    hf = h_v[...].astype(F32)
    rs = lax.rsqrt(jnp.mean(hf * hf, axis=-1, keepdims=True) + EPS)
    lna = lna_v[...].astype(F32)
    for j in range(16):
        sl = slice(j * 128, (j + 1) * 128)
        x_v[:, sl] = (hf[:, sl] * rs * lna[j:j + 1, :]).astype(BF)

    srow = lax.broadcasted_iota(jnp.int32, (S, 128), 0)
    lens = jnp.zeros((S, 128), jnp.int32)
    for s in range(S):
        lens = jnp.where(srow == s, sl_s[s], lens)
    ang = lens.astype(F32) * freq_v[...]
    sgn = jnp.where(lax.broadcasted_iota(jnp.int32, (S, 128), 1) < 64, -1.0, 1.0)
    cos = jnp.cos(ang)
    sin = jnp.sin(ang) * sgn
    trig_v[0] = cos
    trig_v[1] = sin
    for b in range(4):
        col = lax.broadcasted_iota(jnp.int32, (S, 128), 1) + b * 128
        ok = ((col >> 5) == srow) & ((col & 31) <= lens)
        mask_v[:, b * 128:(b + 1) * 128] = jnp.where(ok, 0.0, -1e30)

    x = x_v[...]
    kg = kg_v[...].astype(F32)
    kvw[0].wait()
    kp = jnp.dot(x, wk_v[...], preferred_element_type=F32)
    for g in range(NKV):
        kn_v[0, g] = rms_rope(kp[:, g * 128:(g + 1) * 128], kg, cos, sin)
    kvw[1].wait()
    vp = jnp.dot(x, wv_v[...], preferred_element_type=F32)
    for g in range(NKV):
        kn_v[1, g] = vp[:, g * 128:(g + 1) * 128]

    wq_copy(3).start()

    ri = lax.broadcasted_iota(jnp.int32, (256, 64), 0)
    ci = lax.broadcasted_iota(jnp.int32, (256, 64), 1)
    rep1 = jnp.where(((ri >> 4) == (ci & 15)) & ((ri & 3) == (ci >> 4)), 1.0, 0.0).astype(BF)
    pr = lax.broadcasted_iota(jnp.int32, (128, 128), 0)
    pc = lax.broadcasted_iota(jnp.int32, (128, 128), 1)
    perm = jnp.where(((pr & 31) == (pc >> 2)) & ((pr >> 5) == (pc & 3)), 1.0, 0.0).astype(BF)
    trow = pr >> 2
    for i, (buf, dst) in enumerate(((kc_v, kp_v), (vc_v, vp_v))):
        caches[i].wait()
        rows = buf.reshape(S * T * NKV, HD)
        new = jnp.concatenate([kn_v[i, g].astype(BF) for g in range(NKV)], axis=0)
        rep = jnp.dot(rep1, new, preferred_element_type=F32)
        for s in range(S):
            old = rows[s * 128:(s + 1) * 128, :].astype(F32)
            rep_s = jnp.concatenate([rep[s * 16:(s + 1) * 16, :]] * 8, axis=0)
            upd = jnp.where(trow == sl_s[s], rep_s, old).astype(BF)
            rows[s * 128:(s + 1) * 128, :] = upd
            grp = jnp.dot(perm, upd, preferred_element_type=F32).astype(BF)
            for g in range(NKV):
                dst[g, s * 32:(s + 1) * 32, :] = grp[g * 32:(g + 1) * 32, :]

    def at_copy(g):
        return pltpu.make_async_remote_copy(at_v.at[g, pl.ds(0, S)], at_v.at[g, pl.ds(S, S)], as_sem.at[g], ar_sem.at[g],
                                            device_id={"ep": mate}, device_id_type=MESH)

    qg = qg_v[...].astype(F32)

    def attend(g, q):
        sc = lax.dot_general(q, kp_v[g], (((1,), (1,)), ((), ())), preferred_element_type=F32)
        mk = mask_v[...]
        sc = jnp.where(jnp.concatenate([mk] * GQ, axis=0) == 0.0, sc * (HD ** -0.5), -1e30)
        ex = jnp.exp(sc - jnp.max(sc, axis=-1, keepdims=True))
        pb = (ex / jnp.sum(ex, axis=-1, keepdims=True)).astype(BF)
        o = jnp.dot(pb, vp_v[g], preferred_element_type=F32).astype(BF)
        for j in range(GQ):
            at_v[g, 0:S, j * 128:(j + 1) * 128] = o[j * S:(j + 1) * S, :]

    prev = None
    for g in range(NKV):
        wq_copy(g).wait()
        if g == 0:
            wo_copy(0).start()
            wo_copy(1).start()
        elif g < 3:
            wo_copy(g + 1).start()
        else:
            wr_c.start()
            we_c[0].start()
        q = jnp.dot(x_v[...], wq_v[g], preferred_element_type=F32)
        if g:
            attend(g - 1, prev)
        q = jnp.concatenate([q[:, j * 128:(j + 1) * 128] for j in range(GQ)], axis=0)
        cs = jnp.concatenate([trig_v[0]] * GQ, axis=0)
        sn = jnp.concatenate([trig_v[1]] * GQ, axis=0)
        prev = rms_rope(q, qg, cs, sn).astype(BF)
        if g == 1:
            pl.semaphore_wait(bar, N - 1)
        if g:
            at_copy(g - 1).start()
    wo_copy(0).wait()
    at_copy(0).wait()
    yn = jnp.dot(at_v[0], wo_v[0], preferred_element_type=F32)
    attend(3, prev)
    at_copy(3).start()
    we_c[1].start()

    for g in range(1, NKV):
        wo_copy(g).wait()
        at_copy(g).wait()
        if g == 1:
            we_c[2].start()
        if g < NKV - 1:
            yn = yn + jnp.dot(at_v[g], wo_v[g], preferred_element_type=F32)
    ycps = []
    for n in range(2):
        cols = slice(n * 512, (n + 1) * 512)
        yc = yn[:, cols] + jnp.dot(at_v[NKV - 1], wo_v[NKV - 1, :, cols], preferred_element_type=F32)
        yh_v[half, :, cols] = yc[0:S]
        yp_v[:, cols] = yc[S:2 * S]
        ycps.append(pltpu.make_async_remote_copy(yp_v.at[:, pl.ds(n * 512, 512)], yh_v.at[half, :, pl.ds(n * 512, 512)],
                                                 ys_sem.at[n], yr_sem.at[n], device_id={"ep": mate}, device_id_type=MESH))
        ycps[n].start()

    mc, mx, my, mz = me % 2, me // 2 % 4, me // 8 % 4, me // 32

    def expert_at(slot):
        o, u = (((slot >> 1) & 7) * MUL) & (N - 1), (slot >> 4) * STEP
        return (((((mz + (u >> 2) + (o >> 5)) & 3) * 4 + ((my + u + (o >> 3)) & 3)) * 4 + ((mx + (o >> 1)) & 3)) * 2
                + ((mc + o) & 1))
    slot = lax.broadcasted_iota(jnp.int32, (CAP * N, S), 0)
    e_col = expert_at(slot)
    ids = ids_v[...]
    chosen = jnp.zeros((CAP * N, S), F32)
    for k in range(8):
        chosen = chosen + jnp.where(ids[k:k + 1, :] == e_col, 1.0, 0.0)
    tri = jnp.where(lax.broadcasted_iota(jnp.int32, (S, S), 0) < lax.broadcasted_iota(jnp.int32, (S, S), 1), 1.0, 0.0)
    rank = jnp.dot(chosen.astype(BF), tri.astype(BF), preferred_element_type=F32)
    send = chosen * jnp.where(rank == (slot & 1).astype(F32), 1.0, 0.0)
    snd_v[...] = jnp.transpose(send)
    p_v[...] = send.astype(BF)

    for c in ycps:
        c.wait()
    y = h_v[...].astype(F32) + jnp.concatenate([yh_v[0], yh_v[1]], axis=1)
    y_v[...] = y
    rs = lax.rsqrt(jnp.mean(y * y, axis=-1, keepdims=True) + EPS)
    lnm = lnm_v[...].astype(F32)
    for j in range(16):
        sl = slice(j * 128, (j + 1) * 128)
        r_v[:, sl] = (y[:, sl] * rs * lnm[j:j + 1, :]).astype(BF)

    sview, rview = sbuf.reshape(16, CAP * N, HD), rbuf.reshape(16, CAP * N, HD)
    oview, bview = obuf.reshape(16, CAP * N, HD), bbuf.reshape(16, CAP * N, HD)

    def push(src, dst, s_sem, r_sem, t, sign):
        for i, to in enumerate(peers(me, t, sign)):
            if not (isinstance(t, int) and t * 8 + i == 0):
                k = t * 8 + i
                pltpu.make_async_remote_copy(src.at[:, k], dst.at[:, k], s_sem, r_sem, device_id={"ep": to}, device_id_type=MESH).start()

    def push_group(src, dst, s_sem, r_sem, q, sign):
        if GROUPS[q][0] == 0:
            push(src, dst, s_sem, r_sem, 0, sign)

        @pl.loop(max(1, GROUPS[q][0]), GROUPS[q][1])
        def _(t):
            push(src, dst, s_sem, r_sem, t, sign)
    for q in range(GRP):
        r0, r1 = GROUPS[q][0] * 8 * CAP, GROUPS[q][1] * 8 * CAP
        for n in range(4):
            rows = jnp.dot(p_v[r0:r1, :], r_v[:, n * 512:(n + 1) * 512], preferred_element_type=F32).astype(BF)
            for j in range(4):
                sview[n * 4 + j, r0:r1, :] = rows[:, j * 128:(j + 1) * 128]
        push_group(sbuf, rbuf, ssem, rsem.at[q], q, 1)
    rbuf[:, 0] = sbuf[:, 0]

    wr_c.wait()
    logits = jnp.dot(r_v[...], wr_v[...], preferred_element_type=F32)
    e2 = expert_at(lax.broadcasted_iota(jnp.int32, (N, CAP * N), 1))
    expand = jnp.where(lax.broadcasted_iota(jnp.int32, (N, CAP * N), 0) == e2, 1.0, 0.0)
    lg = jnp.dot(logits, expand, precision=lax.Precision.HIGHEST, preferred_element_type=F32)
    on = snd_v[...] > 0.5
    top = jnp.max(jnp.where(on, lg, -jnp.inf), axis=-1, keepdims=True)
    ex = jnp.where(on, jnp.exp(jnp.where(on, lg - top, 0.0)), 0.0)
    gates = ex / jnp.sum(ex, axis=-1, keepdims=True)
    g1 = gates.astype(BF)
    d1 = gates - g1.astype(F32)
    g2 = d1.astype(BF)
    g3 = (d1 - g2.astype(F32)).astype(BF)
    g_v[...] = jnp.concatenate([g1, g2, g3], axis=0)
    for c in we_c:
        c.wait()

    for q in range(GRP):
        lo, hi = max(1, GROUPS[q][0] * 8), GROUPS[q][1] * 8
        r0, r1 = GROUPS[q][0] * 8 * CAP, hi * CAP
        got = rbuf.at[:, pl.ds(lo, hi - lo)]
        cp(got, got, rsem.at[q]).wait()

        for n in range(FF // 256):
            cols = slice(n * 256, (n + 1) * 256)
            ga = jnp.zeros((r1 - r0, 256), F32)
            ua = jnp.zeros((r1 - r0, 256), F32)
            for kk in range(8):
                xk = jnp.concatenate([rview[2 * kk, r0:r1, :], rview[2 * kk + 1, r0:r1, :]], axis=1)
                ga = ga + jnp.dot(xk, wg_v[kk * 256:(kk + 1) * 256, cols], preferred_element_type=F32)
                ua = ua + jnp.dot(xk, wu_v[kk * 256:(kk + 1) * 256, cols], preferred_element_type=F32)
            hid_v[r0:r1, cols] = (jax.nn.silu(ga) * ua).astype(BF)

        for n in range(4):
            cols = slice(n * 512, (n + 1) * 512)
            o = jnp.dot(hid_v[r0:r1, :], wd_v[:, cols], preferred_element_type=F32).astype(BF)
            for j in range(4):
                oview[n * 4 + j, r0:r1, :] = o[:, j * 128:(j + 1) * 128]

        push_group(obuf, bbuf, osem, bsem.at[q], q, -1)
        if q == 0:
            bbuf[:, 0] = obuf[:, 0]

    for q in range(GRP):
        lo, hi = max(1, GROUPS[q][0] * 8), GROUPS[q][1] * 8
        r0, r1 = GROUPS[q][0] * 8 * CAP, hi * CAP
        got = bbuf.at[:, pl.ds(lo, hi - lo)]
        cp(got, got, bsem.at[q]).wait()
        for n in range(4):
            back = jnp.concatenate([bview[n * 4 + j, r0:r1, :] for j in range(4)], axis=1)
            m = jnp.dot(g_v[:, r0:r1], back, preferred_element_type=F32)
            cols = slice(n * 512, (n + 1) * 512)
            tot = y_v[:, cols] + (m[0:S] + m[S:2 * S] + m[2 * S:3 * S])
            if q + 1 < GRP:
                y_v[:, cols] = tot
            else:
                out_ref[:, cols] = tot.astype(BF)
    sent = sbuf.at[:, pl.ds(1, N - 1)]
    cp(sent, sent, ssem).wait()
    cp(sent, sent, osem).wait()


def finish(a_ref, b_ref, c_ref, a_out, b_out, c_out, sems):
    copies = [pltpu.make_async_copy(x, y, sems.at[i]) for i, (x, y) in enumerate(((a_ref, a_out), (b_ref, b_out), (c_ref, c_out)))]
    for c in copies:
        c.start()
    for c in copies:
        c.wait()


def solution(mesh):
    row_spec = P(('dp', 'ep'), None)
    cache_spec = P(('dp', 'ep'), None, None, None)
    len_spec = P(('dp', 'ep'))
    rep_vec = P(None)
    rep_mat = P(None, None)
    exp_spec = P('ep', None, None)
    inv = np.power(ROPE_BASE, -np.arange(0, HD, 2).astype(np.float32) / HD).astype(np.float32)
    freq_np = np.concatenate([inv, inv])[None, :]
    dma = pltpu.SemaphoreType.DMA

    def local_step(hidden, k_cache, v_cache, seq_lens, expert_ids, ln_attn, w_q, w_k, w_v, q_gain, k_gain, w_o, ln_moe, w_router, w_gate, w_up, w_down):
        anyspec = pl.BlockSpec(memory_space=pl.ANY)
        V = pltpu.VMEM
        made = pl.pallas_call(
            kernel,
            out_shape=(V((S, D), BF), V((S, T, NKV, HD), BF), V((S, T, NKV, HD), BF)),
            in_specs=[anyspec] * 18,
            out_specs=(pl.BlockSpec(memory_space=pltpu.VMEM),) * 3,
            scratch_shapes=[
                V((S, D), BF), pltpu.SMEM((S,), jnp.int32), V((8, S), jnp.int32), V((16, 128), BF), V((16, 128), BF),
                V((1, HD), BF), V((1, HD), BF), V((1, HD), F32),
                V((D, 512), BF), V((D, 512), BF), V((4, D, 1024), BF), V((4, 1024, 1024), BF), V((D, N), BF),
                V((D, FF), BF), V((D, FF), BF), V((FF, D), BF),
                V((NKV, S * T, HD), BF), V((NKV, S * T, HD), BF),
                V((S, D), BF), V((2, NKV, S, HD), F32), V((S, S * T), F32), V((2, S, HD), F32), V((NKV, 2 * S, 1024), BF), V((2, S, 1024), F32), V((S, 1024), F32),
                V((S, D), F32), V((S, D), BF), V((CAP * N, S), BF), V((S, CAP * N), F32), V((3 * S, CAP * N), BF),
                V((CAP * N, FF), BF),
                V((16, N, CAP, HD), BF), V((16, N, CAP, HD), BF), V((16, N, CAP, HD), BF), V((16, N, CAP, HD), BF),
                dma((8,)), dma((2,)), dma((2,)), dma((4,)), dma((4,)), dma, dma((3,)), dma((4,)), dma((4,)), dma((2,)), dma((2,)),
                dma, dma, dma((GRP,)), dma((GRP,)),
            ],
            compiler_params=pltpu.CompilerParams(collective_id=0, has_side_effects=True, vmem_limit_bytes=60 * 1024 * 1024),
        )(hidden, k_cache, v_cache, seq_lens, expert_ids.T, ln_attn.reshape(16, 128), w_q, w_k, w_v,
          q_gain.reshape(1, HD), k_gain.reshape(1, HD), w_o, ln_moe.reshape(16, 128), w_router, w_gate, w_up, w_down,
          jnp.asarray(freq_np))
        return pl.pallas_call(
            finish,
            out_shape=(jax.ShapeDtypeStruct((S, D), BF),
                       jax.ShapeDtypeStruct((S, T, NKV, HD), BF), jax.ShapeDtypeStruct((S, T, NKV, HD), BF)),
            in_specs=[pl.BlockSpec(memory_space=pltpu.VMEM)] * 3,
            out_specs=(anyspec,) * 3,
            scratch_shapes=[dma((3,))],
        )(*[pltpu.with_memory_space_constraint(m, pltpu.VMEM) for m in made])

    return jax.shard_map(local_step, mesh=mesh, in_specs=(row_spec, cache_spec, cache_spec, len_spec, row_spec, rep_vec, rep_mat, rep_mat, rep_mat, rep_vec, rep_vec, rep_mat, rep_vec, rep_mat, exp_spec, exp_spec, exp_spec), out_specs=(row_spec, cache_spec, cache_spec), check_vma=False)
```
